8 devices in a mesh: dp: 2 (over z, y), stage: 4 (over x, core).
Axes of the slice: x: 2, y: 2, z: 1, core: 2. Of those that a mesh axis runs over, the one named last changes fastest.
Arguments:
- token_ids: int32 [32, 512], P('dp'), parts along dimension 0
- label_ids: int32 [32, 512], P('dp'), parts along dimension 0
- embedding: bfloat16 [50304, 768], P('stage')
- w_in: bfloat16 [4, 768, 3072], P('stage')
- w_out: bfloat16 [4, 3072, 768], P('stage')
Outputs:
- output 1: float32 [2], P('dp'), parts along dimension 0
- output 2: float32 [8, 768, 3072], P(('dp', 'stage')), parts along dimension 0
- output 3: float32 [8, 3072, 768], P(('dp', 'stage')), parts along dimension 0
- output 4: float32 [100608, 768], P(('dp', 'stage')), parts along dimension 0
There are 2 independent parts. The reference program is written for one: setup_inputs(seed, part) draws one part's arguments, and reference() takes and returns one part's arrays. A program takes and returns all parts, laid end to end along the dimension named above; an argument that names none is the same for every part.
All inputs are finite; a program needn't handle non-finite values.
Results may differ from the reference program's by a relative error of at most 0.00981087.
Values are sent between devices in bfloat16 or wider.
A program may use at most 1 GiB of HBM per device.

```python
import functools
import jax
import jax.numpy as jnp
from jax import lax

VOCAB_SIZE = 50304
MODEL_DIM = 768
FFN_DIM = 3072
STAGES = 4
MICROBATCHES = 16
MICRO_TOKENS = 512
HOT_IDS = 64
NORM_EPS = 1e-6


def draw_ids(hot_ids, id_key):
    key_pick, key_unif, key_mix = jax.random.split(id_key, 3)
    shape_ids = (MICROBATCHES, MICRO_TOKENS)
    picked = hot_ids[jax.random.randint(key_pick, shape_ids, 0, HOT_IDS)]
    uniform_ids = jax.random.randint(key_unif, shape_ids, 0, VOCAB_SIZE)
    use_hot = jax.random.randint(key_mix, shape_ids, 0, 2) == 1
    return jnp.where(use_hot, picked, uniform_ids).astype(jnp.int32)


def setup_inputs(seed: int = 0, part: int = 0) -> dict:
    root_key = jax.random.key(seed)
    key_ids, key_emb, key_in, key_out = jax.random.split(root_key, 4)
    part_key = jax.random.fold_in(key_ids, part)
    key_hot, key_tok, key_lab = jax.random.split(part_key, 3)
    hot_ids = jax.random.randint(key_hot, (HOT_IDS,), 0, VOCAB_SIZE)
    token_ids = draw_ids(hot_ids, key_tok)
    label_ids = draw_ids(hot_ids, key_lab)
    embedding = jax.random.normal(key_emb, (VOCAB_SIZE, MODEL_DIM), jnp.float32).astype(jnp.bfloat16)
    w_in = (jax.random.normal(key_in, (STAGES, MODEL_DIM, FFN_DIM), jnp.float32) * MODEL_DIM ** -0.5).astype(jnp.bfloat16)
    w_out = (jax.random.normal(key_out, (STAGES, FFN_DIM, MODEL_DIM), jnp.float32) * 2.0 * (FFN_DIM * STAGES) ** -0.5).astype(jnp.bfloat16)
    return {"token_ids": token_ids, "label_ids": label_ids, "embedding": embedding, "w_in": w_in, "w_out": w_out}


def rms_normed(act_rows):
    acts_f = act_rows.astype(jnp.float32)
    return (acts_f * lax.rsqrt(jnp.mean(acts_f * acts_f, axis=-1, keepdims=True) + NORM_EPS)).astype(jnp.bfloat16)


def summed_loss(emb_f32, w_in_f32, w_out_f32, token_ids, label_ids):
    logit_scale = MODEL_DIM ** -0.5
    vocab_iota = jnp.arange(VOCAB_SIZE, dtype=jnp.int32)

    def layer_step(act_rows, weights):
        w_first, w_second = weights
        acts_f = act_rows.astype(jnp.float32)
        pre_act = jnp.dot(acts_f, w_first, preferred_element_type=jnp.float32)
        hidden = jax.nn.gelu(pre_act).astype(jnp.bfloat16)
        out_f = acts_f + jnp.dot(hidden.astype(jnp.float32), w_second, preferred_element_type=jnp.float32)
        return out_f.astype(jnp.bfloat16), None

    def micro_step(loss_total, ids_pair):
        tok_row, lab_row = ids_pair
        act_rows = emb_f32[tok_row].astype(jnp.bfloat16)
        act_rows, _ = lax.scan(layer_step, act_rows, (w_in_f32, w_out_f32))
        normed = rms_normed(act_rows).astype(jnp.float32)
        logits = jnp.dot(normed, emb_f32.T, preferred_element_type=jnp.float32) * logit_scale
        picked = jnp.sum(jnp.where(lab_row[:, None] == vocab_iota[None, :], logits, 0.0), axis=1)
        return loss_total + jnp.sum(jax.nn.logsumexp(logits, axis=1) - picked), None

    loss_total, _ = lax.scan(jax.checkpoint(micro_step), jnp.zeros((), jnp.float32), (token_ids, label_ids))
    return loss_total


def reference(token_ids, label_ids, embedding, w_in, w_out):
    loss_fn = functools.partial(summed_loss, token_ids=token_ids, label_ids=label_ids)
    loss_total, pull_back = jax.vjp(loss_fn, embedding.astype(jnp.float32), w_in.astype(jnp.float32), w_out.astype(jnp.float32))
    grad_emb, grad_in, grad_out = pull_back(jnp.ones((), jnp.float32))
    mean_loss = (loss_total / (MICROBATCHES * MICRO_TOKENS)).reshape(1)
    return (mean_loss, grad_in, grad_out, grad_emb)
```

```python
import functools
import jax
import jax.numpy as jnp
from jax import lax
from jax.experimental import pallas as pl
from jax.experimental.pallas import tpu as pltpu
from jax.sharding import PartitionSpec as P

NORM_EPS = 1e-6
LOG2E = 1.4426950408889634
LN2 = 0.6931471805599453
GELU_K = 0.7978845608028654
GELU_A = 0.044715
SUB = 256
SUBS = 10
TILE = SUB * SUBS
GROUPS = 4
PARTS = 4
V_TILE = 640
VMEM_CAP = 56 * 1024 * 1024
BF = jnp.bfloat16
F32 = jnp.float32
NT = (((1,), (1,)), ((), ()))


def norm_f32(act_rows):
    acts_f = act_rows.astype(F32)
    return acts_f * lax.rsqrt(jnp.mean(acts_f * acts_f, axis=-1, keepdims=True) + NORM_EPS)


def alloc(*shapes):
    return pl.pallas_call(
        lambda *refs: None,
        out_specs=[pl.BlockSpec(memory_space=pl.ANY)] * len(shapes),
        out_shape=[jax.ShapeDtypeStruct(s, BF) for s in shapes],
        name="alloc",
    )()


def layer_forward_body(flags, moved_ref, here_ref, far_ref, w1_ref, w2_ref, _a, _b, _c, out_ref, save_ref, last_ref, n_ref, acc_ref):
    step = pl.program_id(0)

    @pl.when(flags[1] == 1)
    def _():
        @pl.when((step == 0) & (flags[2] == 1))
        def _():
            save_ref[0] = here_ref[0] + far_ref[...]

        @pl.when((step == 0) & (flags[2] == 0))
        def _():
            save_ref[0] = moved_ref[...]

        x = save_ref[0]
        width = w1_ref.shape[1] // PARTS
        total = None
        for part in range(PARTS):
            cols = slice(part * width, (part + 1) * width)
            pre = jnp.dot(x, w1_ref[:, cols], preferred_element_type=F32)
            inner = jnp.tanh(pre * (GELU_K + (GELU_K * GELU_A) * (pre * pre)))
            half = 0.5 * pre
            hidden = (half + half * inner).astype(BF)
            term = jnp.dot(hidden, w2_ref[cols, :], preferred_element_type=F32)
            total = term if total is None else total + term

        @pl.when(step == 0)
        def _():
            acc_ref[...] = total

        @pl.when(step > 0)
        def _():
            acc_ref[...] += total

        @pl.when(step == pl.num_programs(0) - 1)
        def _():
            out = (x.astype(F32) + acc_ref[...]).astype(BF)
            out_ref[...] = out
            last_ref[0] = out
            n_ref[0] = norm_f32(out).astype(BF)


def layer_forward(flags, moved, chip_rows, far, w1, w2, saved_in, last_out, normed, f_tile=1024):
    rows, dim = moved.shape
    ffn = w1.shape[1]
    any_spec = pl.BlockSpec(memory_space=pl.ANY)
    flat = pl.BlockSpec((rows, dim), lambda f, fl: (0, 0))
    slot = pl.BlockSpec((1, rows, dim), lambda f, fl: (fl[0], 0, 0))
    grid_spec = pltpu.PrefetchScalarGridSpec(
        num_scalar_prefetch=1,
        grid=(ffn // f_tile,),
        in_specs=[
            flat,
            pl.BlockSpec((1, rows, dim), lambda f, fl: (fl[3], 0, 0)),
            flat,
            pl.BlockSpec((dim, f_tile), lambda f, fl: (0, f * fl[1])),
            pl.BlockSpec((f_tile, dim), lambda f, fl: (f * fl[1], 0)),
            any_spec, any_spec, any_spec,
        ],
        out_specs=[flat, slot, slot, slot],
        scratch_shapes=[pltpu.VMEM((rows, dim), F32)],
    )
    return pl.pallas_call(
        layer_forward_body,
        grid_spec=grid_spec,
        out_shape=[jax.ShapeDtypeStruct((rows, dim), BF)] + [jax.ShapeDtypeStruct(saved_in.shape, BF)] * 3,
        input_output_aliases={6: 1, 7: 2, 8: 3},
        compiler_params=pltpu.CompilerParams(vmem_limit_bytes=VMEM_CAP),
        cost_estimate=pl.CostEstimate(flops=4 * rows * dim * ffn, bytes_accessed=4 * dim * ffn, transcendentals=rows * ffn),
        name="layer_fwd",
    )(flags, moved, chip_rows, far, w1, w2, saved_in, last_out, normed)


def head_forward_body(n_valid, log_scale, n_ref, e_ref, lab_ref, p_ref, m_ref, st_ref, run):
    tile, chunk = pl.program_id(0), pl.program_id(1)

    @pl.when(tile == 0)
    def _():
        run[chunk, 0:1, :] = jnp.full((1, run.shape[2]), -jnp.inf, F32)
        run[chunk, 1:3, :] = jnp.zeros((2, run.shape[2]), F32)

    n_rows = n_ref[0]
    lab = lab_ref[0] - tile * TILE
    top, tot, hit = run[chunk, 0:1, :], run[chunk, 1:2, :], run[chunk, 2:3, :]
    rows = lax.broadcasted_iota(jnp.int32, (SUB, n_rows.shape[0]), 0)
    for sub in range(SUBS):
        cut = slice(sub * SUB, (sub + 1) * SUB)
        logit = lax.dot_general(e_ref[cut, :], n_rows, NT, preferred_element_type=F32) * log_scale
        if sub == SUBS - 1:
            logit = jnp.where(rows < n_valid - tile * TILE - sub * SUB, logit, -jnp.inf)
        hit = hit + jnp.sum(jnp.where(rows == lab - sub * SUB, logit, 0.0), axis=0, keepdims=True)
        new_top = jnp.maximum(top, jnp.max(logit, axis=0, keepdims=True))
        expo = jnp.exp2(logit - new_top)
        tot = tot * jnp.exp2(top - new_top) + jnp.sum(expo, axis=0, keepdims=True)
        p_ref[0, cut, :] = expo.astype(BF)
        m_ref[0, 0, sub:sub + 1, :] = new_top
        top = new_top
    run[chunk, 0:1, :] = top
    run[chunk, 1:2, :] = tot
    run[chunk, 2:3, :] = hit
    st_ref[0, 0:1, :] = top
    st_ref[0, 1:2, :] = tot
    st_ref[0, 2:3, :] = hit


def head_forward(normed, emb_pad, labels, n_valid, log_scale):
    chunks, rows, dim = normed.shape
    padded = emb_pad.shape[0]
    tiles = padded // TILE
    row = pl.BlockSpec((1, 1, rows), lambda t, c: (c, 0, 0))
    return pl.pallas_call(
        functools.partial(head_forward_body, n_valid, log_scale),
        grid=(tiles, chunks),
        in_specs=[
            pl.BlockSpec((1, rows, dim), lambda t, c: (c, 0, 0)),
            pl.BlockSpec((TILE, dim), lambda t, c: (t, 0)),
            row,
        ],
        out_specs=[
            pl.BlockSpec((1, TILE, rows), lambda t, c: (c, t, 0)),
            pl.BlockSpec((1, 1, SUBS, rows), lambda t, c: (c, t, 0, 0)),
            pl.BlockSpec((1, 3, rows), lambda t, c: (c, 0, 0)),
        ],
        out_shape=[
            jax.ShapeDtypeStruct((chunks, padded, rows), BF),
            jax.ShapeDtypeStruct((chunks, tiles, SUBS, rows), F32),
            jax.ShapeDtypeStruct((chunks, 3, rows), F32),
        ],
        scratch_shapes=[pltpu.VMEM((chunks, 3, rows), F32)],
        compiler_params=pltpu.CompilerParams(vmem_limit_bytes=VMEM_CAP),
        cost_estimate=pl.CostEstimate(flops=2 * chunks * rows * dim * padded, bytes_accessed=padded * (2 * dim + 2 * rows * chunks), transcendentals=rows * chunks * padded),
        name="head_fwd",
    )(normed, emb_pad, labels)


def head_backward_body(p_ref, c_ref, lab_ref, g_ref, et_ref, d_ref, out_ref, acc_ref):
    tile, chunk = pl.program_id(0), pl.program_id(1)
    lab = lab_ref[0] - tile * TILE
    gain = g_ref[0]
    rows = lax.broadcasted_iota(jnp.int32, (SUB, lab.shape[1]), 0)
    total = None
    for sub in range(SUBS):
        cut = slice(sub * SUB, (sub + 1) * SUB)
        prob = p_ref[0, cut, :].astype(F32) * c_ref[0, 0, sub:sub + 1, :]
        delta = jnp.where(rows == lab - sub * SUB, gain, prob).astype(BF)
        d_ref[0, cut, :] = delta
        term = jnp.dot(et_ref[:, cut], delta, preferred_element_type=F32)
        total = term if total is None else total + term

    @pl.when(tile == 0)
    def _():
        acc_ref[chunk] = total

    @pl.when(tile > 0)
    def _():
        acc_ref[chunk] += total

    @pl.when(tile == pl.num_programs(0) - 1)
    def _():
        out_ref[0] = acc_ref[chunk].T.astype(BF)


def head_backward(expo, coef, labels, gain, emb_t):
    chunks, padded, rows = expo.shape
    dim = emb_t.shape[0]
    tiles = padded // TILE
    row = pl.BlockSpec((1, 1, rows), lambda t, c: (c, 0, 0))
    block = pl.BlockSpec((1, TILE, rows), lambda t, c: (c, t, 0))
    end = tiles - 1
    return pl.pallas_call(
        head_backward_body,
        grid=(tiles, chunks),
        in_specs=[
            block,
            pl.BlockSpec((1, 1, SUBS, rows), lambda t, c: (c, t, 0, 0)),
            row,
            row,
            pl.BlockSpec((dim, TILE), lambda t, c: (0, t)),
        ],
        out_specs=[block, pl.BlockSpec((1, rows, dim), lambda t, c: (c * (t // end), 0, 0))],
        out_shape=[jax.ShapeDtypeStruct(expo.shape, BF), jax.ShapeDtypeStruct((chunks, rows, dim), BF)],
        scratch_shapes=[pltpu.VMEM((chunks, dim, rows), F32)],
        input_output_aliases={0: 0},
        compiler_params=pltpu.CompilerParams(vmem_limit_bytes=VMEM_CAP),
        cost_estimate=pl.CostEstimate(flops=2 * chunks * rows * dim * padded, bytes_accessed=padded * (2 * dim + 4 * rows * chunks), transcendentals=0),
        name="head_bwd",
    )(expo, coef, labels, gain, emb_t)


def table_grad_body(groups, *refs):
    deltas, normed, out_ref = refs[:groups], refs[groups:2 * groups], refs[2 * groups]
    total = None
    for d_ref, n_ref in zip(deltas, normed):
        for chunk in range(d_ref.shape[0]):
            term = jnp.dot(d_ref[chunk], n_ref[chunk], preferred_element_type=F32)
            total = term if total is None else total + term
    out_ref[...] = total


def table_grad(deltas, normed, slice_rows, v_tile):
    chunks, rows, dim = normed[0].shape
    groups = len(deltas)
    tokens = groups * chunks * rows
    return pl.pallas_call(
        functools.partial(table_grad_body, groups),
        grid=(-(-slice_rows // v_tile),),
        in_specs=[pl.BlockSpec((chunks, v_tile, rows), lambda v: (0, v, 0))] * groups
        + [pl.BlockSpec((chunks, rows, dim), lambda v: (0, 0, 0), pipeline_mode=pl.Buffered(1))] * groups,
        out_specs=pl.BlockSpec((v_tile, dim), lambda v: (v, 0)),
        out_shape=jax.ShapeDtypeStruct((slice_rows, dim), F32),
        compiler_params=pltpu.CompilerParams(vmem_limit_bytes=VMEM_CAP),
        cost_estimate=pl.CostEstimate(flops=2 * slice_rows * dim * tokens, bytes_accessed=2 * slice_rows * tokens, transcendentals=0),
        name="table_grad",
    )(*deltas, *normed)


def layer_backward_body(flags, x_ref, moved_ref, top_ref, mdx_ref, w1_ref, w2_ref, _a, _b, _c, _d, gin_ref, g_ref, h_ref, gp_ref, dx_ref, acc_ref):
    step = pl.program_id(0)
    end = pl.num_programs(0) - 1

    @pl.when((step == end) & (flags[4] == 0))
    def _():
        dx_ref[0] = mdx_ref[...]

    @pl.when(flags[1] == 1)
    def _():
        @pl.when((step == 0) & (flags[2] == 1))
        def _():
            g_ref[0] = top_ref[0]

        @pl.when((step == 0) & (flags[2] == 0))
        def _():
            g_ref[0] = moved_ref[...]

        x = x_ref[0]
        grad_out = g_ref[0]
        width = w1_ref.shape[1] // PARTS
        total = None
        for part in range(PARTS):
            cols = slice(part * width, (part + 1) * width)
            pre = jnp.dot(x, w1_ref[:, cols], preferred_element_type=F32)
            grad_hidden = lax.dot_general(grad_out, w2_ref[cols, :], NT, preferred_element_type=F32)
            sq = pre * pre
            inner = jnp.tanh(pre * (GELU_K + (GELU_K * GELU_A) * sq))
            side = 0.5 + 0.5 * inner
            bend = (0.5 - 0.5 * inner * inner) * (GELU_K + (3.0 * GELU_K * GELU_A) * sq)
            h_ref[0, :, cols] = (pre * side).astype(BF)
            grad_pre = (grad_hidden * (side + pre * bend)).astype(BF)
            gp_ref[0, :, cols] = grad_pre
            term = lax.dot_general(grad_pre, w1_ref[:, cols], NT, preferred_element_type=F32)
            total = term if total is None else total + term

        @pl.when(step == 0)
        def _():
            acc_ref[...] = total

        @pl.when(step > 0)
        def _():
            acc_ref[...] += total

        @pl.when(step == end)
        def _():
            grad_in = (grad_out.astype(F32) + acc_ref[...]).astype(BF)
            gin_ref[...] = grad_in

            @pl.when(flags[4] == 1)
            def _():
                dx_ref[0] = grad_in


def layer_backward(flags, saved_in, moved, grad_last, moved_dx, w1, w2, grads, hidden, grad_pre, dx_all, f_tile=768):
    rows, dim = moved.shape
    ffn = w1.shape[1]
    any_spec = pl.BlockSpec(memory_space=pl.ANY)
    wide = pl.BlockSpec((1, rows, f_tile), lambda f, fl: (fl[0], 0, f * fl[1]))
    flat = pl.BlockSpec((rows, dim), lambda f, fl: (0, 0))
    slot = pl.BlockSpec((1, rows, dim), lambda f, fl: (fl[0], 0, 0))
    grid_spec = pltpu.PrefetchScalarGridSpec(
        num_scalar_prefetch=1,
        grid=(ffn // f_tile,),
        in_specs=[
            slot,
            flat,
            pl.BlockSpec((1, rows, dim), lambda f, fl: (fl[3], 0, 0)),
            flat,
            pl.BlockSpec((dim, f_tile), lambda f, fl: (0, f * fl[1])),
            pl.BlockSpec((f_tile, dim), lambda f, fl: (f * fl[1], 0)),
            any_spec, any_spec, any_spec, any_spec,
        ],
        out_specs=[flat, slot, wide, wide, pl.BlockSpec((1, rows, dim), lambda f, fl: (fl[5], 0, 0))],
        scratch_shapes=[pltpu.VMEM((rows, dim), F32)],
    )
    return pl.pallas_call(
        layer_backward_body,
        grid_spec=grid_spec,
        out_shape=[jax.ShapeDtypeStruct((rows, dim), BF)] + [jax.ShapeDtypeStruct(a.shape, BF) for a in (grads, hidden, grad_pre, dx_all)],
        input_output_aliases={7: 1, 8: 2, 9: 3, 10: 4},
        compiler_params=pltpu.CompilerParams(vmem_limit_bytes=VMEM_CAP),
        cost_estimate=pl.CostEstimate(flops=6 * rows * dim * ffn, bytes_accessed=4 * dim * ffn + 4 * rows * ffn, transcendentals=rows * ffn),
        name="layer_bwd",
    )(flags, saved_in, moved, grad_last, moved_dx, w1, w2, grads, hidden, grad_pre, dx_all)


def take(store, slot):
    return lax.dynamic_index_in_dim(store, slot, 0, keepdims=False)


def solution(mesh):
    n_stage = mesh.shape["stage"]
    last = n_stage - 1
    fwd_pairs = [(src, src + 1) for src in range(last)]
    bwd_pairs = [(src + 1, src) for src in range(last)]

    def stage_body(token_ids, label_ids, emb_rows, w_in, w_out):
        stage = lax.axis_index("stage")
        is_first = (stage == 0).astype(jnp.int32)
        is_last = (stage == last).astype(jnp.int32)
        micro_count, micro_tokens = token_ids.shape
        slice_rows, dim = emb_rows.shape
        ffn = w_in.shape[2]
        scale = dim ** -0.5
        w1, w2 = w_in[0], w_out[0]
        row_start = stage * slice_rows
        padded = -(-slice_rows // TILE) * TILE
        spare = micro_count
        per = micro_count // GROUPS

        def hop(value, *pairs):
            return lax.ppermute(value, "stage", pairs)

        def place(idx):
            active = (idx >= 0) & (idx < micro_count)
            return jnp.where(active, idx, spare), active.astype(jnp.int32), jnp.clip(idx, 0, micro_count - 1)

        local_tok = token_ids - row_start
        tok_here = (local_tok >= 0) & (local_tok < slice_rows)
        looked_up = jnp.take(emb_rows, jnp.clip(local_tok, 0, slice_rows - 1), axis=0)
        own_rows = jnp.where(tok_here[..., None], looked_up, 0)
        chip_rows = own_rows + hop(own_rows, (1, 0), (3, 2))

        emb_pad = jnp.pad(emb_rows, ((0, padded - slice_rows), (0, 0)))
        emb_t = emb_pad.T
        local_lab = label_ids - row_start
        labels = jnp.where((local_lab >= 0) & (local_lab < slice_rows), local_lab, -1)[:, None]

        act_zero = jnp.zeros((micro_tokens, dim), BF)
        store = (micro_count + 1, micro_tokens, dim)
        wide = (micro_count + 1, micro_tokens, ffn)
        saved_in, last_out, normed, grads, dx_all, hidden, grad_pre = alloc(store, store, store, store, store, wide, wide)

        def far_rows(idx):
            return hop(take(chip_rows, jnp.minimum(idx, micro_count - 1)), (2, 0))

        def fwd_tick(tick, carry):
            moved, far, out, saved_in, last_out, normed = carry
            next_moved = lax.ppermute(out, "stage", fwd_pairs)
            next_far = far_rows(tick + 1)
            slot, active, idx = place(tick - 2 * stage)
            flags = jnp.stack([slot, active, is_first, idx])
            out, saved_in, last_out, normed = layer_forward(flags, moved, chip_rows, far, w1, w2, saved_in, last_out, normed)
            return next_moved, next_far, out, saved_in, last_out, normed

        carry = (act_zero, far_rows(0), act_zero, saved_in, last_out, normed)
        carry = lax.fori_loop(0, micro_count + 2 * last, fwd_tick, carry)
        _, _, _, saved_in, last_out, normed = carry

        cuts = [slice(g * per, (g + 1) * per) for g in range(GROUPS)]
        n_parts, expo, maxes, stats = [], [], [], []
        for cut in cuts:
            own = normed[cut]
            near = hop(own, (3, 2))
            cross = hop(own, (3, 1))
            final = hop(cross, (1, 0))
            part = jnp.where(stage == 3, own, jnp.where(stage == 2, near, jnp.where(stage == 1, cross, final)))
            n_parts.append(part)
            res = head_forward(part, emb_pad, labels[cut], slice_rows, scale * LOG2E)
            expo.append(res[0])
            maxes.append(res[1])
            stats.append(res[2])

        every = lax.all_gather(jnp.concatenate(stats), "stage")
        top = jnp.max(every[:, :, 0], axis=0)
        denom = jnp.sum(every[:, :, 1] * jnp.exp2(every[:, :, 0] - top), axis=0)
        hit = jnp.sum(every[:, :, 2], axis=0)
        mean_loss = (jnp.sum(jnp.log2(denom) + top - hit) * (LN2 / (micro_count * micro_tokens))).reshape(1)
        ratio = scale / denom
        gain = ((jnp.exp2(hit - top) / denom - 1.0) * scale)[:, None]

        deltas, grad_last = [], []
        for g, cut in enumerate(cuts):
            coef = jnp.exp2(maxes[g] - top[cut, None, None]) * ratio[cut, None, None]
            delta, part = head_backward(expo[g], coef, labels[cut], gain[cut], emb_t)
            deltas.append(delta)
            near = hop(part, (0, 1), (2, 3)).astype(F32)
            pair = part.astype(F32) + near
            far = hop(pair.astype(BF), (1, 3)).astype(F32)
            _, pull = jax.vjp(norm_f32, last_out[cut])
            grad_last.append(pull(pair + far)[0])
        grad_last = jnp.concatenate(grad_last)

        grad_head = table_grad(deltas, n_parts, slice_rows, V_TILE)

        def bwd_tick(tick, carry):
            moved, moved_dx, grad_in, grads, hidden, grad_pre, dx_all = carry
            next_moved = lax.ppermute(grad_in, "stage", bwd_pairs)
            next_dx = hop(grad_in, (0, 2))
            slot, active, idx = place(tick - 2 * (last - stage))
            dx_slot, _, _ = place(tick - 2 * last - 2 + 2 * is_first)
            flags = jnp.stack([slot, active, is_last, idx, is_first, dx_slot])
            grad_in, grads, hidden, grad_pre, dx_all = layer_backward(
                flags, saved_in, moved, grad_last, moved_dx, w1, w2, grads, hidden, grad_pre, dx_all)
            return next_moved, next_dx, grad_in, grads, hidden, grad_pre, dx_all

        carry = (act_zero, act_zero, act_zero, grads, hidden, grad_pre, dx_all)
        carry = lax.fori_loop(0, micro_count + 2 * last + 2, bwd_tick, carry)
        _, _, _, grads, hidden, grad_pre, dx_all = carry

        def clear(value):
            blank = jnp.zeros((1,) + value.shape[1:], BF)
            return lax.dynamic_update_slice(value, blank, (spare, 0, 0)).reshape(-1, value.shape[2])

        grad_first = jnp.einsum("td,tf->df", clear(saved_in), clear(grad_pre), preferred_element_type=F32)
        grad_second = jnp.einsum("tf,td->fd", clear(hidden), clear(grads), preferred_element_type=F32)
        dx_rows = dx_all[:micro_count]
        dx_rows = jnp.where(stage % 2 == 0, dx_rows, hop(dx_rows, (0, 1), (2, 3)))
        seg = jnp.where(tok_here, local_tok, slice_rows).reshape(-1)
        grad_emb = grad_head.at[seg].add(dx_rows.reshape(-1, dim).astype(F32), mode="drop")
        return mean_loss, grad_first[None], grad_second[None], grad_emb

    return jax.shard_map(
        stage_body,
        mesh=mesh,
        in_specs=(P("dp", None), P("dp", None), P("stage", None), P("stage", None, None), P("stage", None, None)),
        out_specs=(P("dp"), P(("dp", "stage"), None, None), P(("dp", "stage"), None, None), P(("dp", "stage"), None)),
        check_vma=False,
    )
```

```python
import functools
import jax
import jax.numpy as jnp
from jax import lax
from jax.experimental import pallas as pl
from jax.experimental.pallas import tpu as pltpu
from jax.sharding import PartitionSpec as P

NORM_EPS = 1e-6
LOG2E = 1.4426950408889634
LN2 = 0.6931471805599453
GELU_K = 0.7978845608028654
GELU_A = 0.044715
SUB = 512
SUBS = 5
STAGES = 4
MESH = pl.DeviceIdType.MESH
PIPE_CAP = 60 * 1024 * 1024
TILE = SUB * SUBS
GROUPS = 4
PARTS = 6
V_TILE = 640
VMEM_CAP = 56 * 1024 * 1024
BF = jnp.bfloat16
F32 = jnp.float32


def norm_f32(act_rows):
    acts_f = act_rows.astype(F32)
    return acts_f * lax.rsqrt(jnp.mean(acts_f * acts_f, axis=-1, keepdims=True) + NORM_EPS)


def gelu_hidden(pre):
    inner = jnp.tanh(pre * (GELU_K + (GELU_K * GELU_A) * (pre * pre)))
    half = 0.5 * pre
    return (half + half * inner).astype(BF)


def remote(src, dst, send_sem, recv_sem, target):
    return pltpu.make_async_remote_copy(src_ref=src, dst_ref=dst, send_sem=send_sem, recv_sem=recv_sem,
                                        device_id=(lax.axis_index("dp"), target), device_id_type=MESH)


def forward_pipe_body(here_ref, w1_ref, w2_ref, save_ref, last_ref, n_ref, recv, local, out_buf, w1, w2,
                      w_sem, local_sem, recv_sem, send_sem, far_sem, save_sem, last_sem, n_sem):
    stage = lax.axis_index("stage")
    count = recv.shape[0]
    end = STAGES - 1
    ffn = w1.shape[1]
    width = ffn // PARTS
    loads = [pltpu.make_async_copy(w1_ref, w1, w_sem.at[0]), pltpu.make_async_copy(w2_ref, w2, w_sem.at[1])]
    for load in loads:
        load.start()

    def far(m):
        return remote(here_ref.at[m], recv.at[m], far_sem.at[m], recv_sem.at[m], 0)

    def onward(m):
        return remote(out_buf.at[m], recv.at[m], send_sem.at[m], recv_sem.at[m], lax.rem(stage + 1, STAGES))

    def begin(m, _):
        @pl.when(stage == 2)
        def _():
            far(m).start()

        @pl.when(stage == 0)
        def _():
            pltpu.make_async_copy(here_ref.at[m], local.at[m], local_sem.at[m]).start()
        return 0

    lax.fori_loop(0, count, begin, 0)
    for load in loads:
        load.wait()

    def chunk(m, _):
        onward(m).wait_recv()

        @pl.when(stage == 0)
        def _():
            pltpu.make_async_copy(here_ref.at[m], local.at[m], local_sem.at[m]).wait()
            recv[m] = recv[m] + local[m]

        pltpu.make_async_copy(recv.at[m], save_ref.at[m], save_sem.at[m]).start()
        x = recv[m]
        total = None
        for part in range(PARTS):
            cols = slice(part * width, (part + 1) * width)
            hidden = gelu_hidden(jnp.dot(x, w1[:, cols], preferred_element_type=F32))
            term = jnp.dot(hidden, w2[cols, :], preferred_element_type=F32)
            total = term if total is None else total + term
        out_buf[m] = (x.astype(F32) + total).astype(BF)

        @pl.when(stage < end)
        def _():
            onward(m).start()

        @pl.when(stage == end)
        def _():
            local[m] = norm_f32(out_buf[m]).astype(BF)
            pltpu.make_async_copy(out_buf.at[m], last_ref.at[m], last_sem.at[m]).start()
            pltpu.make_async_copy(local.at[m], n_ref.at[m], n_sem.at[m]).start()
        return 0

    lax.fori_loop(0, count, chunk, 0)

    def finish(m, _):
        pltpu.make_async_copy(recv.at[m], save_ref.at[m], save_sem.at[m]).wait()

        @pl.when(stage == 2)
        def _():
            far(m).wait_send()

        @pl.when(stage < end)
        def _():
            onward(m).wait_send()

        @pl.when(stage == end)
        def _():
            pltpu.make_async_copy(out_buf.at[m], last_ref.at[m], last_sem.at[m]).wait()
            pltpu.make_async_copy(local.at[m], n_ref.at[m], n_sem.at[m]).wait()
        return 0

    lax.fori_loop(0, count, finish, 0)


def forward_pipe(chip_rows, w1, w2):
    count, rows, dim = chip_rows.shape
    any_spec = pl.BlockSpec(memory_space=pl.ANY)
    store = jax.ShapeDtypeStruct(chip_rows.shape, BF)
    dma = pltpu.SemaphoreType.DMA
    return pl.pallas_call(
        forward_pipe_body,
        in_specs=[any_spec] * 3,
        out_specs=[any_spec] * 3,
        out_shape=[store] * 3,
        scratch_shapes=[pltpu.VMEM(chip_rows.shape, BF)] * 3 + [pltpu.VMEM(w1.shape, BF), pltpu.VMEM(w2.shape, BF), dma((2,))] + [dma((count,))] * 7,
        compiler_params=pltpu.CompilerParams(vmem_limit_bytes=PIPE_CAP, has_side_effects=True),
        cost_estimate=pl.CostEstimate(flops=4 * count * rows * dim * w1.shape[1], bytes_accessed=4 * dim * w1.shape[1], transcendentals=0),
        name="forward_pipe",
    )(chip_rows, w1, w2)


def backward_pipe_body(x_ref, top_ref, w1_ref, w1t_ref, w2t_ref, g_ref, h_ref, gp_ref, dx_ref, recv, x_buf, h_buf, gp_buf, gin_buf, w1, w1t, w2t,
                       w_sem, top_sem, x_sem, recv_sem, send_sem, g_sem, h_sem, gp_sem, dx_sem, dx_recv):
    stage = lax.axis_index("stage")
    count = recv.shape[0]
    end = STAGES - 1
    width = w1.shape[1] // PARTS
    loads = [pltpu.make_async_copy(src, dst, w_sem.at[i]) for i, (src, dst) in enumerate(((w1_ref, w1), (w1t_ref, w1t), (w2t_ref, w2t)))]
    for load in loads:
        load.start()

    def load_top(m):
        return pltpu.make_async_copy(top_ref.at[m], recv.at[m], top_sem.at[m])

    def load_x(m):
        return pltpu.make_async_copy(x_ref.at[m], x_buf.at[lax.rem(m, 2)], x_sem.at[m])

    def save_g(m):
        return pltpu.make_async_copy(recv.at[m], g_ref.at[m], g_sem.at[m])

    def save_h(m):
        return pltpu.make_async_copy(h_buf.at[lax.rem(m, 2)], h_ref.at[m], h_sem.at[m])

    def save_gp(m):
        return pltpu.make_async_copy(gp_buf.at[lax.rem(m, 2)], gp_ref.at[m], gp_sem.at[m])

    def save_dx(m):
        return pltpu.make_async_copy(gin_buf.at[lax.rem(m, 2)], dx_ref.at[m], dx_sem.at[m])

    def onward(m):
        return remote(gin_buf.at[lax.rem(m, 2)], recv.at[m], send_sem.at[m], recv_sem.at[m], lax.rem(stage + end, STAGES))

    def cross(m):
        return remote(gin_buf.at[lax.rem(m, 2)], dx_ref.at[m], send_sem.at[m], dx_recv.at[m], 2)

    def begin(m, _):
        @pl.when(stage == end)
        def _():
            load_top(m).start()
        return 0

    lax.fori_loop(0, count, begin, 0)
    load_x(0).start()
    for load in loads:
        load.wait()

    def drain(m):
        save_h(m).wait()
        save_gp(m).wait()

        @pl.when(stage > 0)
        def _():
            onward(m).wait_send()

        @pl.when(stage == 0)
        def _():
            cross(m).wait_send()
            save_dx(m).wait()

    def chunk(m, _):
        slot = lax.rem(m, 2)

        @pl.when(m + 1 < count)
        def _():
            load_x(m + 1).start()

        @pl.when(stage == end)
        def _():
            load_top(m).wait()

        @pl.when(stage < end)
        def _():
            onward(m).wait_recv()

        save_g(m).start()
        load_x(m).wait()

        @pl.when(m >= 2)
        def _():
            drain(m - 2)

        x = x_buf[slot]
        grad_out = recv[m]
        total = None
        for part in range(PARTS):
            cols = slice(part * width, (part + 1) * width)
            pre = jnp.dot(x, w1[:, cols], preferred_element_type=F32)
            grad_hidden = jnp.dot(grad_out, w2t[:, cols], preferred_element_type=F32)
            sq = pre * pre
            inner = jnp.tanh(pre * (GELU_K + (GELU_K * GELU_A) * sq))
            side = 0.5 + 0.5 * inner
            bend = (0.5 - 0.5 * inner * inner) * (GELU_K + (3.0 * GELU_K * GELU_A) * sq)
            h_buf[slot, :, cols] = (pre * side).astype(BF)
            grad_pre = (grad_hidden * (side + pre * bend)).astype(BF)
            gp_buf[slot, :, cols] = grad_pre
            term = jnp.dot(grad_pre, w1t[cols, :], preferred_element_type=F32)
            total = term if total is None else total + term
        gin_buf[slot] = (grad_out.astype(F32) + total).astype(BF)
        save_h(m).start()
        save_gp(m).start()

        @pl.when(stage > 0)
        def _():
            onward(m).start()

        @pl.when(stage == 0)
        def _():
            cross(m).start()
            save_dx(m).start()
        return 0

    lax.fori_loop(0, count, chunk, 0)
    drain(count - 2)
    drain(count - 1)

    def finish(m, _):
        save_g(m).wait()

        @pl.when(stage == 2)
        def _():
            cross(m).wait_recv()
        return 0

    lax.fori_loop(0, count, finish, 0)


def backward_pipe(saved_in, grad_last, w1, w1t, w2t):
    count, rows, dim = saved_in.shape
    ffn = w1.shape[1]
    any_spec = pl.BlockSpec(memory_space=pl.ANY)
    store = jax.ShapeDtypeStruct(saved_in.shape, BF)
    wide = jax.ShapeDtypeStruct((count, rows, ffn), BF)
    dma = pltpu.SemaphoreType.DMA
    return pl.pallas_call(
        backward_pipe_body,
        in_specs=[any_spec] * 5,
        out_specs=[any_spec] * 4,
        out_shape=[store, wide, wide, store],
        scratch_shapes=[
            pltpu.VMEM(saved_in.shape, BF),
            pltpu.VMEM((2, rows, dim), BF),
            pltpu.VMEM((2, rows, ffn), BF),
            pltpu.VMEM((2, rows, ffn), BF),
            pltpu.VMEM((2, rows, dim), BF),
            pltpu.VMEM(w1.shape, BF), pltpu.VMEM(w1t.shape, BF), pltpu.VMEM(w2t.shape, BF),
            dma((3,)),
        ] + [dma((count,))] * 9,
        compiler_params=pltpu.CompilerParams(vmem_limit_bytes=PIPE_CAP, has_side_effects=True),
        cost_estimate=pl.CostEstimate(flops=6 * count * rows * dim * ffn, bytes_accessed=4 * dim * ffn, transcendentals=0),
        name="backward_pipe",
    )(saved_in, grad_last, w1, w1t, w2t)


def head_forward_body(n_valid, log_scale, n_ref, e_ref, lab_ref, p_ref, m_ref, st_ref, run):
    tile, chunk = pl.program_id(0), pl.program_id(1)

    @pl.when(tile == 0)
    def _():
        run[chunk, 0:1, :] = jnp.full((1, run.shape[2]), -jnp.inf, F32)
        run[chunk, 1:3, :] = jnp.zeros((2, run.shape[2]), F32)

    n_rows = n_ref[0]
    lab = lab_ref[0] - tile * TILE
    top, tot, hit = run[chunk, 0:1, :], run[chunk, 1:2, :], run[chunk, 2:3, :]
    rows = lax.broadcasted_iota(jnp.int32, (SUB, n_rows.shape[1]), 0)
    for sub in range(SUBS):
        cut = slice(sub * SUB, (sub + 1) * SUB)
        logit = jnp.dot(e_ref[cut, :], n_rows, preferred_element_type=F32) * log_scale
        if sub == SUBS - 1:
            logit = jnp.where(rows < n_valid - tile * TILE - sub * SUB, logit, -jnp.inf)
        hit = hit + jnp.sum(jnp.where(rows == lab - sub * SUB, logit, 0.0), axis=0, keepdims=True)
        new_top = jnp.maximum(top, jnp.max(logit, axis=0, keepdims=True))
        expo = jnp.exp2(logit - new_top)
        tot = tot * jnp.exp2(top - new_top) + jnp.sum(expo, axis=0, keepdims=True)
        p_ref[0, cut, :] = expo.astype(BF)
        m_ref[0, 0, sub:sub + 1, :] = new_top
        top = new_top
    run[chunk, 0:1, :] = top
    run[chunk, 1:2, :] = tot
    run[chunk, 2:3, :] = hit
    st_ref[0, 0:1, :] = top
    st_ref[0, 1:2, :] = tot
    st_ref[0, 2:3, :] = hit


def head_forward(normed, emb_pad, labels, n_valid, log_scale):
    chunks, dim, rows = normed.shape
    padded = emb_pad.shape[0]
    tiles = padded // TILE
    row = pl.BlockSpec((1, 1, rows), lambda t, c: (c, 0, 0))
    return pl.pallas_call(
        functools.partial(head_forward_body, n_valid, log_scale),
        grid=(tiles, chunks),
        in_specs=[
            pl.BlockSpec((1, dim, rows), lambda t, c: (c, 0, 0)),
            pl.BlockSpec((TILE, dim), lambda t, c: (t, 0)),
            row,
        ],
        out_specs=[
            pl.BlockSpec((1, TILE, rows), lambda t, c: (c, t, 0)),
            pl.BlockSpec((1, 1, SUBS, rows), lambda t, c: (c, t, 0, 0)),
            pl.BlockSpec((1, 3, rows), lambda t, c: (c, 0, 0)),
        ],
        out_shape=[
            jax.ShapeDtypeStruct((chunks, padded, rows), BF),
            jax.ShapeDtypeStruct((chunks, tiles, SUBS, rows), F32),
            jax.ShapeDtypeStruct((chunks, 3, rows), F32),
        ],
        scratch_shapes=[pltpu.VMEM((chunks, 3, rows), F32)],
        compiler_params=pltpu.CompilerParams(vmem_limit_bytes=VMEM_CAP),
        cost_estimate=pl.CostEstimate(flops=2 * chunks * rows * dim * padded, bytes_accessed=padded * (2 * dim + 2 * rows * chunks), transcendentals=rows * chunks * padded),
        name="head_fwd",
    )(normed, emb_pad, labels)


def head_backward_body(p_ref, c_ref, lab_ref, g_ref, et_ref, d_ref, out_ref, acc_ref):
    tile, chunk = pl.program_id(0), pl.program_id(1)
    lab = lab_ref[0] - tile * TILE
    gain = g_ref[0]
    rows = lax.broadcasted_iota(jnp.int32, (SUB, lab.shape[1]), 0)
    total = None
    for sub in range(SUBS):
        cut = slice(sub * SUB, (sub + 1) * SUB)
        prob = p_ref[0, cut, :].astype(F32) * c_ref[0, 0, sub:sub + 1, :]
        delta = jnp.where(rows == lab - sub * SUB, gain, prob).astype(BF)
        d_ref[0, cut, :] = delta
        term = jnp.dot(et_ref[:, cut], delta, preferred_element_type=F32)
        total = term if total is None else total + term

    @pl.when(tile == 0)
    def _():
        acc_ref[chunk] = total

    @pl.when(tile > 0)
    def _():
        acc_ref[chunk] += total

    @pl.when(tile == pl.num_programs(0) - 1)
    def _():
        out_ref[0] = acc_ref[chunk].T.astype(BF)


def head_backward(expo, coef, labels, gain, emb_t):
    chunks, padded, rows = expo.shape
    dim = emb_t.shape[0]
    tiles = padded // TILE
    row = pl.BlockSpec((1, 1, rows), lambda t, c: (c, 0, 0))
    block = pl.BlockSpec((1, TILE, rows), lambda t, c: (c, t, 0))
    end = tiles - 1
    return pl.pallas_call(
        head_backward_body,
        grid=(tiles, chunks),
        in_specs=[
            block,
            pl.BlockSpec((1, 1, SUBS, rows), lambda t, c: (c, t, 0, 0)),
            row,
            row,
            pl.BlockSpec((dim, TILE), lambda t, c: (0, t)),
        ],
        out_specs=[block, pl.BlockSpec((1, rows, dim), lambda t, c: (c * (t // end), 0, 0))],
        out_shape=[jax.ShapeDtypeStruct(expo.shape, BF), jax.ShapeDtypeStruct((chunks, rows, dim), BF)],
        scratch_shapes=[pltpu.VMEM((chunks, dim, rows), F32)],
        input_output_aliases={0: 0},
        compiler_params=pltpu.CompilerParams(vmem_limit_bytes=VMEM_CAP),
        cost_estimate=pl.CostEstimate(flops=2 * chunks * rows * dim * padded, bytes_accessed=padded * (2 * dim + 4 * rows * chunks), transcendentals=0),
        name="head_bwd",
    )(expo, coef, labels, gain, emb_t)


def table_grad_body(groups, *refs):
    deltas, normed, out_ref = refs[:groups], refs[groups:2 * groups], refs[2 * groups]
    total = None
    for d_ref, n_ref in zip(deltas, normed):
        for chunk in range(d_ref.shape[0]):
            term = jnp.dot(d_ref[chunk], n_ref[chunk], preferred_element_type=F32)
            total = term if total is None else total + term
    out_ref[...] = total


def table_grad(deltas, normed, slice_rows, v_tile):
    chunks, rows, dim = normed[0].shape
    groups = len(deltas)
    tokens = groups * chunks * rows
    return pl.pallas_call(
        functools.partial(table_grad_body, groups),
        grid=(-(-slice_rows // v_tile),),
        in_specs=[pl.BlockSpec((chunks, v_tile, rows), lambda v: (0, v, 0))] * groups
        + [pl.BlockSpec((chunks, rows, dim), lambda v: (0, 0, 0), pipeline_mode=pl.Buffered(1))] * groups,
        out_specs=pl.BlockSpec((v_tile, dim), lambda v: (v, 0)),
        out_shape=jax.ShapeDtypeStruct((slice_rows, dim), F32),
        compiler_params=pltpu.CompilerParams(vmem_limit_bytes=VMEM_CAP),
        cost_estimate=pl.CostEstimate(flops=2 * slice_rows * dim * tokens, bytes_accessed=2 * slice_rows * tokens, transcendentals=0),
        name="table_grad",
    )(*deltas, *normed)


def solution(mesh):

    def stage_body(token_ids, label_ids, emb_rows, w_in, w_out):
        stage = lax.axis_index("stage")
        micro_count, micro_tokens = token_ids.shape
        slice_rows, dim = emb_rows.shape
        scale = dim ** -0.5
        w1, w2 = w_in[0], w_out[0]
        row_start = stage * slice_rows
        padded = -(-slice_rows // TILE) * TILE
        per = micro_count // GROUPS

        def hop(value, *pairs):
            return lax.ppermute(value, "stage", pairs)

        local_tok = token_ids - row_start
        tok_here = (local_tok >= 0) & (local_tok < slice_rows)
        looked_up = jnp.take(emb_rows, jnp.clip(local_tok, 0, slice_rows - 1), axis=0)
        own_rows = jnp.where(tok_here[..., None], looked_up, 0)
        chip_rows = own_rows + hop(own_rows, (1, 0), (3, 2))

        emb_pad = jnp.pad(emb_rows, ((0, padded - slice_rows), (0, 0)))
        emb_t = emb_pad.T
        local_lab = label_ids - row_start
        labels = jnp.where((local_lab >= 0) & (local_lab < slice_rows), local_lab, -1)[:, None]

        saved_in, last_out, normed = forward_pipe(chip_rows, w1, w2)

        cuts = [slice(g * per, (g + 1) * per) for g in range(GROUPS)]
        n_parts, expo, maxes, stats = [], [], [], []
        for cut in cuts:
            own = normed[cut]
            near = hop(own, (3, 2))
            cross = hop(own, (3, 1))
            final = hop(cross, (1, 0))
            part = jnp.where(stage == 3, own, jnp.where(stage == 2, near, jnp.where(stage == 1, cross, final)))
            n_parts.append(part)
            res = head_forward(part.transpose(0, 2, 1), emb_pad, labels[cut], slice_rows, scale * LOG2E)
            expo.append(res[0])
            maxes.append(res[1])
            stats.append(res[2])

        every = lax.all_gather(jnp.concatenate(stats), "stage")
        top = jnp.max(every[:, :, 0], axis=0)
        denom = jnp.sum(every[:, :, 1] * jnp.exp2(every[:, :, 0] - top), axis=0)
        hit = jnp.sum(every[:, :, 2], axis=0)
        mean_loss = (jnp.sum(jnp.log2(denom) + top - hit) * (LN2 / (micro_count * micro_tokens))).reshape(1)
        ratio = scale / denom
        gain = ((jnp.exp2(hit - top) / denom - 1.0) * scale)[:, None]

        deltas, grad_last = [], []
        for g, cut in enumerate(cuts):
            coef = jnp.exp2(maxes[g] - top[cut, None, None]) * ratio[cut, None, None]
            delta, part = head_backward(expo[g], coef, labels[cut], gain[cut], emb_t)
            deltas.append(delta)
            near = hop(part, (0, 1), (2, 3)).astype(F32)
            pair = part.astype(F32) + near
            far = hop(pair.astype(BF), (1, 3)).astype(F32)
            _, pull = jax.vjp(norm_f32, last_out[cut])
            grad_last.append(pull(pair + far)[0])
        grad_last = jnp.concatenate(grad_last)

        grad_head = table_grad(deltas, n_parts, slice_rows, V_TILE)

        grads, hidden, grad_pre, dx_rows = backward_pipe(saved_in, grad_last, w1, w1.T, w2.T)

        def flat(value):
            return value.reshape(-1, value.shape[2])

        grad_first = jnp.einsum("td,tf->df", flat(saved_in), flat(grad_pre), preferred_element_type=F32)
        grad_second = jnp.einsum("tf,td->fd", flat(hidden), flat(grads), preferred_element_type=F32)
        dx_rows = jnp.where(stage % 2 == 0, dx_rows, hop(dx_rows, (0, 1), (2, 3)))
        seg = jnp.where(tok_here, local_tok, slice_rows).reshape(-1)
        grad_emb = grad_head.at[seg].add(dx_rows.reshape(-1, dim).astype(F32), mode="drop")
        return mean_loss, grad_first[None], grad_second[None], grad_emb

    return jax.shard_map(
        stage_body,
        mesh=mesh,
        in_specs=(P("dp", None), P("dp", None), P("stage", None), P("stage", None, None), P("stage", None, None)),
        out_specs=(P("dp"), P(("dp", "stage"), None, None), P(("dp", "stage"), None, None), P(("dp", "stage"), None)),
        check_vma=False,
    )
```

```python
import functools
import jax
import jax.numpy as jnp
from jax import lax
from jax.experimental import pallas as pl
from jax.experimental.pallas import tpu as pltpu
from jax.sharding import PartitionSpec as P

NORM_EPS = 1e-6
GELU_K = 0.7978845608028654
GELU_A = 0.044715
SUB = 256
SUBS = 10
STAGES = 4
MESH = pl.DeviceIdType.MESH
PIPE_CAP = 60 * 1024 * 1024
TILE = SUB * SUBS
CUTS = (0, 2, 6, 11, 16)
PARTS = 6
V_TILE = 640
VMEM_CAP = 56 * 1024 * 1024
BF = jnp.bfloat16
F32 = jnp.float32


def norm_f32(act_rows):
    acts_f = act_rows.astype(F32)
    return acts_f * lax.rsqrt(jnp.mean(acts_f * acts_f, axis=-1, keepdims=True) + NORM_EPS)


def gelu_hidden(pre):
    inner = jnp.tanh(pre * (GELU_K + (GELU_K * GELU_A) * (pre * pre)))
    half = 0.5 * pre
    return (half + half * inner).astype(BF)


def remote(src, dst, send_sem, recv_sem, target):
    return pltpu.make_async_remote_copy(src_ref=src, dst_ref=dst, send_sem=send_sem, recv_sem=recv_sem,
                                        device_id=(lax.axis_index("dp"), target), device_id_type=MESH)


def forward_pipe_body(here_ref, w1_ref, w2_ref, save_ref, last_ref, n_ref, recv, local, out_buf, w1, w2,
                      w_sem, local_sem, recv_sem, send_sem, far_sem, save_sem, last_sem, n_sem):
    stage = lax.axis_index("stage")
    count = recv.shape[0]
    end = STAGES - 1
    ffn = w1.shape[1]
    width = ffn // PARTS
    loads = [pltpu.make_async_copy(w1_ref, w1, w_sem.at[0]), pltpu.make_async_copy(w2_ref, w2, w_sem.at[1])]
    for load in loads:
        load.start()

    def far(m):
        return remote(here_ref.at[m], recv.at[m], far_sem.at[m], recv_sem.at[m], 0)

    def onward(m):
        return remote(out_buf.at[m], recv.at[m], send_sem.at[m], recv_sem.at[m], lax.rem(stage + 1, STAGES))

    def begin(m, _):
        @pl.when(stage == 2)
        def _():
            far(m).start()

        @pl.when(stage == 0)
        def _():
            pltpu.make_async_copy(here_ref.at[m], local.at[m], local_sem.at[m]).start()
        return 0

    lax.fori_loop(0, count, begin, 0)
    for load in loads:
        load.wait()

    def chunk(m, _):
        onward(m).wait_recv()

        @pl.when(stage == 0)
        def _():
            pltpu.make_async_copy(here_ref.at[m], local.at[m], local_sem.at[m]).wait()
            recv[m] = recv[m] + local[m]

        pltpu.make_async_copy(recv.at[m], save_ref.at[m], save_sem.at[m]).start()
        x = recv[m]
        total = None
        ahead = jnp.dot(x, w1[:, 0:width], preferred_element_type=F32)
        for part in range(PARTS):
            cols = slice(part * width, (part + 1) * width)
            pre = ahead
            if part < PARTS - 1:
                ahead = jnp.dot(x, w1[:, (part + 1) * width:(part + 2) * width], preferred_element_type=F32)
            hidden = gelu_hidden(pre)
            term = jnp.dot(hidden, w2[cols, :], preferred_element_type=F32)
            total = term if total is None else total + term
        out_buf[m] = (x.astype(F32) + total).astype(BF)

        @pl.when(stage < end)
        def _():
            onward(m).start()

        @pl.when(stage == end)
        def _():
            local[m] = norm_f32(out_buf[m]).astype(BF)
            pltpu.make_async_copy(out_buf.at[m], last_ref.at[m], last_sem.at[m]).start()
            pltpu.make_async_copy(local.at[m], n_ref.at[m], n_sem.at[m]).start()
        return 0

    lax.fori_loop(0, count, chunk, 0)

    def finish(m, _):
        pltpu.make_async_copy(recv.at[m], save_ref.at[m], save_sem.at[m]).wait()

        @pl.when(stage == 2)
        def _():
            far(m).wait_send()

        @pl.when(stage < end)
        def _():
            onward(m).wait_send()

        @pl.when(stage == end)
        def _():
            pltpu.make_async_copy(out_buf.at[m], last_ref.at[m], last_sem.at[m]).wait()
            pltpu.make_async_copy(local.at[m], n_ref.at[m], n_sem.at[m]).wait()
        return 0

    lax.fori_loop(0, count, finish, 0)


def forward_pipe(chip_rows, w1, w2):
    count, rows, dim = chip_rows.shape
    any_spec = pl.BlockSpec(memory_space=pl.ANY)
    store = jax.ShapeDtypeStruct(chip_rows.shape, BF)
    dma = pltpu.SemaphoreType.DMA
    return pl.pallas_call(
        forward_pipe_body,
        in_specs=[any_spec] * 3,
        out_specs=[any_spec] * 3,
        out_shape=[store] * 3,
        scratch_shapes=[pltpu.VMEM(chip_rows.shape, BF)] * 3 + [pltpu.VMEM(w1.shape, BF), pltpu.VMEM(w2.shape, BF), dma((2,))] + [dma((count,))] * 7,
        compiler_params=pltpu.CompilerParams(vmem_limit_bytes=PIPE_CAP, has_side_effects=True),
        cost_estimate=pl.CostEstimate(flops=4 * count * rows * dim * w1.shape[1], bytes_accessed=4 * dim * w1.shape[1], transcendentals=0),
        name="forward_pipe",
    )(chip_rows, w1, w2)


def backward_pipe_body(x_ref, top_ref, w1_ref, w1t_ref, w2t_ref, g_ref, h_ref, gp_ref, dx_ref, recv, x_buf, h_buf, gp_buf, gin_buf, w1, w1t, w2t,
                       w_sem, top_sem, x_sem, recv_sem, send_sem, g_sem, h_sem, gp_sem, dx_sem, dx_recv):
    stage = lax.axis_index("stage")
    count = recv.shape[0]
    end = STAGES - 1
    width = w1.shape[1] // PARTS
    loads = [pltpu.make_async_copy(src, dst, w_sem.at[i]) for i, (src, dst) in enumerate(((w1_ref, w1), (w1t_ref, w1t), (w2t_ref, w2t)))]
    for load in loads:
        load.start()

    def load_top(m):
        return pltpu.make_async_copy(top_ref.at[m], recv.at[m], top_sem.at[m])

    def load_x(m):
        return pltpu.make_async_copy(x_ref.at[m], x_buf.at[lax.rem(m, 2)], x_sem.at[m])

    def save_g(m):
        return pltpu.make_async_copy(recv.at[m], g_ref.at[m], g_sem.at[m])

    def save_h(m):
        return pltpu.make_async_copy(h_buf.at[lax.rem(m, 2)], h_ref.at[m], h_sem.at[m])

    def save_gp(m):
        return pltpu.make_async_copy(gp_buf.at[lax.rem(m, 2)], gp_ref.at[m], gp_sem.at[m])

    def save_dx(m):
        return pltpu.make_async_copy(gin_buf.at[lax.rem(m, 2)], dx_ref.at[m], dx_sem.at[m])

    def onward(m):
        return remote(gin_buf.at[lax.rem(m, 2)], recv.at[m], send_sem.at[m], recv_sem.at[m], lax.rem(stage + end, STAGES))

    def cross(m):
        return remote(gin_buf.at[lax.rem(m, 2)], dx_ref.at[m], send_sem.at[m], dx_recv.at[m], 2)

    def begin(m, _):
        @pl.when(stage == end)
        def _():
            load_top(m).start()
        return 0

    lax.fori_loop(0, count, begin, 0)
    load_x(0).start()
    for load in loads:
        load.wait()

    def drain(m):
        save_h(m).wait()
        save_gp(m).wait()

        @pl.when(stage > 0)
        def _():
            onward(m).wait_send()

        @pl.when(stage == 0)
        def _():
            cross(m).wait_send()
            save_dx(m).wait()

    def chunk(m, _):
        slot = lax.rem(m, 2)

        @pl.when(m + 1 < count)
        def _():
            load_x(m + 1).start()

        @pl.when(stage == end)
        def _():
            load_top(m).wait()

        @pl.when(stage < end)
        def _():
            onward(m).wait_recv()

        save_g(m).start()
        load_x(m).wait()

        @pl.when(m >= 2)
        def _():
            drain(m - 2)

        x = x_buf[slot]
        grad_out = recv[m]

        def both(part):
            cols = slice(part * width, (part + 1) * width)
            return (jnp.dot(x, w1[:, cols], preferred_element_type=F32),
                    jnp.dot(grad_out, w2t[:, cols], preferred_element_type=F32))

        total = None
        ahead = both(0)
        for part in range(PARTS):
            cols = slice(part * width, (part + 1) * width)
            pre, grad_hidden = ahead
            if part < PARTS - 1:
                ahead = both(part + 1)
            sq = pre * pre
            inner = jnp.tanh(pre * (GELU_K + (GELU_K * GELU_A) * sq))
            side = 0.5 + 0.5 * inner
            bend = (0.5 - 0.5 * inner * inner) * (GELU_K + (3.0 * GELU_K * GELU_A) * sq)
            h_buf[slot, :, cols] = (pre * side).astype(BF)
            grad_pre = (grad_hidden * (side + pre * bend)).astype(BF)
            gp_buf[slot, :, cols] = grad_pre
            term = jnp.dot(grad_pre, w1t[cols, :], preferred_element_type=F32)
            total = term if total is None else total + term
        gin_buf[slot] = (grad_out.astype(F32) + total).astype(BF)
        save_h(m).start()
        save_gp(m).start()

        @pl.when(stage > 0)
        def _():
            onward(m).start()

        @pl.when(stage == 0)
        def _():
            cross(m).start()
            save_dx(m).start()
        return 0

    lax.fori_loop(0, count, chunk, 0)
    drain(count - 2)
    drain(count - 1)

    def finish(m, _):
        save_g(m).wait()

        @pl.when(stage == 2)
        def _():
            cross(m).wait_recv()
        return 0

    lax.fori_loop(0, count, finish, 0)


def backward_pipe(saved_in, grad_last, w1, w1t, w2t):
    count, rows, dim = saved_in.shape
    ffn = w1.shape[1]
    any_spec = pl.BlockSpec(memory_space=pl.ANY)
    store = jax.ShapeDtypeStruct(saved_in.shape, BF)
    wide = jax.ShapeDtypeStruct((count, rows, ffn), BF)
    dma = pltpu.SemaphoreType.DMA
    return pl.pallas_call(
        backward_pipe_body,
        in_specs=[any_spec] * 5,
        out_specs=[any_spec] * 4,
        out_shape=[store, wide, wide, store],
        scratch_shapes=[
            pltpu.VMEM(saved_in.shape, BF),
            pltpu.VMEM((2, rows, dim), BF),
            pltpu.VMEM((2, rows, ffn), BF),
            pltpu.VMEM((2, rows, ffn), BF),
            pltpu.VMEM((2, rows, dim), BF),
            pltpu.VMEM(w1.shape, BF), pltpu.VMEM(w1t.shape, BF), pltpu.VMEM(w2t.shape, BF),
            dma((3,)),
        ] + [dma((count,))] * 9,
        compiler_params=pltpu.CompilerParams(vmem_limit_bytes=PIPE_CAP, has_side_effects=True),
        cost_estimate=pl.CostEstimate(flops=6 * count * rows * dim * ffn, bytes_accessed=4 * dim * ffn, transcendentals=0),
        name="backward_pipe",
    )(saved_in, grad_last, w1, w1t, w2t)


def head_forward_body(n_valid, scale, n_ref, e_ref, lab_ref, p_ref, m_ref, st_ref, run):
    tile, chunk = pl.program_id(0), pl.program_id(1)

    @pl.when(tile == 0)
    def _():
        run[chunk, 0:1, :] = jnp.full((1, run.shape[2]), -jnp.inf, F32)
        run[chunk, 1:3, :] = jnp.zeros((2, run.shape[2]), F32)

    n_rows = n_ref[0]
    lab = lab_ref[0] - tile * TILE
    top, tot, hit = run[chunk, 0:1, :], run[chunk, 1:2, :], run[chunk, 2:3, :]
    rows = lax.broadcasted_iota(jnp.int32, (SUB, n_rows.shape[1]), 0)
    for sub in range(SUBS):
        cut = slice(sub * SUB, (sub + 1) * SUB)
        logit = jnp.dot(e_ref[cut, :], n_rows, preferred_element_type=F32) * scale
        if sub == SUBS - 1:
            logit = jnp.where(rows < n_valid - tile * TILE - sub * SUB, logit, -jnp.inf)
        hit = hit + jnp.sum(jnp.where(rows == lab - sub * SUB, logit, 0.0), axis=0, keepdims=True)
        new_top = jnp.maximum(top, jnp.max(logit, axis=0, keepdims=True))
        expo = jnp.exp(logit - new_top)
        tot = tot * jnp.exp(top - new_top) + jnp.sum(expo, axis=0, keepdims=True)
        p_ref[0, cut, :] = expo.astype(BF)
        m_ref[0, 0, sub:sub + 1, :] = new_top
        top = new_top
    run[chunk, 0:1, :] = top
    run[chunk, 1:2, :] = tot
    run[chunk, 2:3, :] = hit
    st_ref[0, 0:1, :] = top
    st_ref[0, 1:2, :] = tot
    st_ref[0, 2:3, :] = hit


def transpose_body(n_valid, e_ref, out_ref):
    rows = lax.broadcasted_iota(jnp.int32, e_ref.shape, 0)
    out_ref[...] = jnp.where(rows < n_valid - pl.program_id(0) * e_ref.shape[0], e_ref[...], 0).T


def transposed_table(emb_rows, padded, width=1280):
    n_valid, dim = emb_rows.shape
    return pl.pallas_call(
        functools.partial(transpose_body, n_valid),
        grid=(padded // width,),
        in_specs=[pl.BlockSpec((width, dim), lambda t: (t, 0))],
        out_specs=pl.BlockSpec((dim, width), lambda t: (0, t)),
        out_shape=jax.ShapeDtypeStruct((dim, padded), BF),
        compiler_params=pltpu.CompilerParams(vmem_limit_bytes=VMEM_CAP),
        cost_estimate=pl.CostEstimate(flops=20 * padded * dim, bytes_accessed=4 * padded * dim, transcendentals=0),
        name="table_t",
    )(emb_rows)


def head_forward(normed, emb_rows, labels, scale):
    chunks, dim, rows = normed.shape
    n_valid = emb_rows.shape[0]
    tiles = -(-n_valid // TILE)
    padded = tiles * TILE
    row = pl.BlockSpec((1, 1, rows), lambda t, c: (c, 0, 0))
    return pl.pallas_call(
        functools.partial(head_forward_body, n_valid, scale),
        grid=(tiles, chunks),
        in_specs=[
            pl.BlockSpec((1, dim, rows), lambda t, c: (c, 0, 0)),
            pl.BlockSpec((TILE, dim), lambda t, c: (t, 0)),
            row,
        ],
        out_specs=[
            pl.BlockSpec((1, TILE, rows), lambda t, c: (c, t, 0)),
            pl.BlockSpec((1, 1, SUBS, rows), lambda t, c: (c, t, 0, 0)),
            pl.BlockSpec((1, 3, rows), lambda t, c: (c, 0, 0)),
        ],
        out_shape=[
            jax.ShapeDtypeStruct((chunks, padded, rows), BF),
            jax.ShapeDtypeStruct((chunks, tiles, SUBS, rows), F32),
            jax.ShapeDtypeStruct((chunks, 3, rows), F32),
        ],
        scratch_shapes=[pltpu.VMEM((chunks, 3, rows), F32)],
        compiler_params=pltpu.CompilerParams(vmem_limit_bytes=VMEM_CAP),
        cost_estimate=pl.CostEstimate(flops=2 * chunks * rows * dim * padded, bytes_accessed=padded * (2 * dim + 2 * rows * chunks), transcendentals=rows * chunks * padded),
        name="head_fwd",
    )(normed, emb_rows, labels)


def head_backward_body(p_ref, c_ref, lab_ref, g_ref, et_ref, d_ref, out_ref, acc_ref):
    tile, chunk = pl.program_id(0), pl.program_id(1)
    lab = lab_ref[0] - tile * TILE
    gain = g_ref[0]
    rows = lax.broadcasted_iota(jnp.int32, (SUB, lab.shape[1]), 0)
    def delta_of(sub):
        cut = slice(sub * SUB, (sub + 1) * SUB)
        prob = p_ref[0, cut, :].astype(F32) * c_ref[0, 0, sub:sub + 1, :]
        delta = jnp.where(rows == lab - sub * SUB, gain, prob).astype(BF)
        d_ref[0, cut, :] = delta
        return delta

    total = None
    ahead = delta_of(0)
    for sub in range(SUBS):
        delta = ahead
        if sub < SUBS - 1:
            ahead = delta_of(sub + 1)
        term = jnp.dot(et_ref[:, sub * SUB:(sub + 1) * SUB], delta, preferred_element_type=F32)
        total = term if total is None else total + term

    @pl.when(tile == 0)
    def _():
        acc_ref[chunk] = total

    @pl.when(tile > 0)
    def _():
        acc_ref[chunk] += total

    @pl.when(tile == pl.num_programs(0) - 1)
    def _():
        out_ref[0] = acc_ref[chunk].T.astype(BF)


def head_backward(expo, coef, labels, gain, emb_t):
    chunks, padded, rows = expo.shape
    dim = emb_t.shape[0]
    tiles = padded // TILE
    row = pl.BlockSpec((1, 1, rows), lambda t, c: (c, 0, 0))
    block = pl.BlockSpec((1, TILE, rows), lambda t, c: (c, t, 0))
    end = tiles - 1
    return pl.pallas_call(
        head_backward_body,
        grid=(tiles, chunks),
        in_specs=[
            block,
            pl.BlockSpec((1, 1, SUBS, rows), lambda t, c: (c, t, 0, 0)),
            row,
            row,
            pl.BlockSpec((dim, TILE), lambda t, c: (0, t)),
        ],
        out_specs=[block, pl.BlockSpec((1, rows, dim), lambda t, c: (c * (t // end), 0, 0))],
        out_shape=[jax.ShapeDtypeStruct(expo.shape, BF), jax.ShapeDtypeStruct((chunks, rows, dim), BF)],
        scratch_shapes=[pltpu.VMEM((chunks, dim, rows), F32)],
        input_output_aliases={0: 0},
        compiler_params=pltpu.CompilerParams(vmem_limit_bytes=VMEM_CAP),
        cost_estimate=pl.CostEstimate(flops=2 * chunks * rows * dim * padded, bytes_accessed=padded * (2 * dim + 4 * rows * chunks), transcendentals=0),
        name="head_bwd",
    )(expo, coef, labels, gain, emb_t)


def table_grad_body(groups, *refs):
    deltas, normed, out_ref = refs[:groups], refs[groups:2 * groups], refs[2 * groups]
    total = None
    for d_ref, n_ref in zip(deltas, normed):
        for chunk in range(d_ref.shape[0]):
            term = jnp.dot(d_ref[chunk], n_ref[chunk], preferred_element_type=F32)
            total = term if total is None else total + term
    out_ref[...] = total


def table_grad(deltas, normed, slice_rows, v_tile):
    _, rows, dim = normed[0].shape
    groups = len(deltas)
    tokens = sum(part.shape[0] for part in normed) * rows
    return pl.pallas_call(
        functools.partial(table_grad_body, groups),
        grid=(-(-slice_rows // v_tile),),
        in_specs=[pl.BlockSpec((part.shape[0], v_tile, rows), lambda v: (0, v, 0)) for part in deltas]
        + [pl.BlockSpec(part.shape, lambda v: (0, 0, 0), pipeline_mode=pl.Buffered(1)) for part in normed],
        out_specs=pl.BlockSpec((v_tile, dim), lambda v: (v, 0)),
        out_shape=jax.ShapeDtypeStruct((slice_rows, dim), F32),
        compiler_params=pltpu.CompilerParams(vmem_limit_bytes=VMEM_CAP),
        cost_estimate=pl.CostEstimate(flops=2 * slice_rows * dim * tokens, bytes_accessed=2 * slice_rows * tokens, transcendentals=0),
        name="table_grad",
    )(*deltas, *normed)


def solution(mesh):

    def stage_body(token_ids, label_ids, emb_rows, w_in, w_out):
        stage = lax.axis_index("stage")
        micro_count, micro_tokens = token_ids.shape
        slice_rows, dim = emb_rows.shape
        scale = dim ** -0.5
        w1, w2 = w_in[0], w_out[0]
        row_start = stage * slice_rows
        padded = -(-slice_rows // TILE) * TILE
        unit = micro_count // CUTS[-1]

        def hop(value, *pairs):
            return lax.ppermute(value, "stage", pairs)

        local_tok = token_ids - row_start
        tok_here = (local_tok >= 0) & (local_tok < slice_rows)
        looked_up = jnp.take(emb_rows, jnp.clip(local_tok, 0, slice_rows - 1), axis=0)
        own_rows = jnp.where(tok_here[..., None], looked_up, 0)
        chip_rows = own_rows + hop(own_rows, (1, 0), (3, 2))

        emb_t = transposed_table(emb_rows, padded)
        local_lab = label_ids - row_start
        labels = jnp.where((local_lab >= 0) & (local_lab < slice_rows), local_lab, -1)[:, None]

        saved_in, last_out, normed = forward_pipe(chip_rows, w1, w2)

        cuts = [slice(lo * unit, hi * unit) for lo, hi in zip(CUTS[:-1], CUTS[1:])]
        n_parts, expo, maxes, stats = [], [], [], []
        for g, cut in enumerate(cuts):
            own = normed[cut]
            if g > 0:
                own, n_parts[-1] = lax.optimization_barrier((own, n_parts[-1]))
            near = hop(own, (3, 2))
            cross = hop(own, (3, 1))
            relay = cross
            if g > 0:
                relay, stats[-1] = lax.optimization_barrier((cross, stats[-1]))
            final = hop(relay, (1, 0))
            part = jnp.where(stage == 3, own, jnp.where(stage == 2, near, jnp.where(stage == 1, relay, final)))
            res = head_forward(part.transpose(0, 2, 1), emb_rows, labels[cut], scale)
            n_parts.append(part)
            expo.append(res[0])
            maxes.append(res[1])
            stats.append(res[2])

        every = lax.all_gather(jnp.concatenate(stats), "stage")
        top = jnp.max(every[:, :, 0], axis=0)
        denom = jnp.sum(every[:, :, 1] * jnp.exp(every[:, :, 0] - top), axis=0)
        hit = jnp.sum(every[:, :, 2], axis=0)
        mean_loss = (jnp.sum(jnp.log(denom) + top - hit) / (micro_count * micro_tokens)).reshape(1)
        ratio = scale / denom
        gain = ((jnp.exp(hit - top) / denom - 1.0) * scale)[:, None]

        deltas, pairs = [], []
        for g, cut in enumerate(cuts):
            coef = jnp.exp(maxes[g] - top[cut, None, None]) * ratio[cut, None, None]
            delta, part = head_backward(expo[g], coef, labels[cut], gain[cut], emb_t)
            if g >= 2:
                part, pairs[g - 2] = lax.optimization_barrier((part, pairs[g - 2]))
            deltas.append(delta)
            pairs.append(part.astype(F32) + hop(part, (0, 1), (2, 3)).astype(F32))
        sent = [pair.astype(BF) for pair in pairs]
        deltas, sent, pairs = lax.optimization_barrier((deltas, sent, pairs))
        far = [hop(value, (1, 3)) for value in sent]
        grad_head = table_grad(deltas, n_parts, slice_rows, V_TILE)
        far, grad_head = lax.optimization_barrier((far, grad_head))
        grad_n = jnp.concatenate([pair + value.astype(F32) for pair, value in zip(pairs, far)])
        _, pull = jax.vjp(norm_f32, last_out)
        grad_last = pull(grad_n)[0]

        grads, hidden, grad_pre, dx_rows = backward_pipe(saved_in, grad_last, w1, w1.T, w2.T)

        def flat(value):
            return value.reshape(-1, value.shape[2])

        grad_first = jnp.einsum("td,tf->df", flat(saved_in), flat(grad_pre), preferred_element_type=F32)
        grad_second = jnp.einsum("tf,td->fd", flat(hidden), flat(grads), preferred_element_type=F32)
        dx_rows = jnp.where(stage % 2 == 0, dx_rows, hop(dx_rows, (0, 1), (2, 3)))
        seg = jnp.where(tok_here, local_tok, slice_rows).reshape(-1)
        grad_emb = grad_head.at[seg].add(dx_rows.reshape(-1, dim).astype(F32), mode="drop")
        return mean_loss, grad_first[None], grad_second[None], grad_emb

    return jax.shard_map(
        stage_body,
        mesh=mesh,
        in_specs=(P("dp", None), P("dp", None), P("stage", None), P("stage", None, None), P("stage", None, None)),
        out_specs=(P("dp"), P(("dp", "stage"), None, None), P(("dp", "stage"), None, None), P(("dp", "stage"), None)),
        check_vma=False,
    )
```

```python
import functools
import jax
import jax.numpy as jnp
from jax import lax
from jax.experimental import pallas as pl
from jax.experimental.pallas import tpu as pltpu
from jax.sharding import PartitionSpec as P

NORM_EPS = 1e-6
LOG2E = 1.4426950408889634
LN2 = 0.6931471805599453
GELU_K = 0.7978845608028654
GELU_A = 0.044715
SUB = 256
SUBS = 10
STAGES = 4
MESH = pl.DeviceIdType.MESH
PIPE_CAP = 60 * 1024 * 1024
TILE = SUB * SUBS
CUTS = (0, 2, 6, 11, 16)
PARTS = 6
SPLIT = 2
V_TILE = 640
VMEM_CAP = 56 * 1024 * 1024
BF = jnp.bfloat16
F32 = jnp.float32
NT = (((1,), (1,)), ((), ()))


def norm_f32(act_rows):
    acts_f = act_rows.astype(F32)
    return acts_f * lax.rsqrt(jnp.mean(acts_f * acts_f, axis=-1, keepdims=True) + NORM_EPS)


def gelu_hidden(pre):
    inner = jnp.tanh(pre * (GELU_K + (GELU_K * GELU_A) * (pre * pre)))
    half = 0.5 * pre
    return (half + half * inner).astype(BF)


def remote(src, dst, send_sem, recv_sem, target):
    return pltpu.make_async_remote_copy(src_ref=src, dst_ref=dst, send_sem=send_sem, recv_sem=recv_sem,
                                        device_id=(lax.axis_index("dp"), target), device_id_type=MESH)


def forward_pipe_body(here_ref, w1_ref, w2_ref, save_ref, last_ref, n_ref, recv, local, out_buf, w1, w2,
                      w_sem, local_sem, recv_sem, send_sem, far_sem, save_sem, last_sem, n_sem):
    stage = lax.axis_index("stage")
    count = recv.shape[0]
    end = STAGES - 1
    ffn = w1.shape[1]
    width = ffn // PARTS
    loads = [pltpu.make_async_copy(w1_ref, w1, w_sem.at[0]), pltpu.make_async_copy(w2_ref, w2, w_sem.at[1])]
    for load in loads:
        load.start()

    def far(m):
        return remote(here_ref.at[m], recv.at[m], far_sem.at[m], recv_sem.at[m], 0)

    def onward(m):
        return remote(out_buf.at[m], recv.at[m], send_sem.at[m], recv_sem.at[m], lax.rem(stage + 1, STAGES))

    def begin(m, _):
        @pl.when(stage == 2)
        def _():
            far(m).start()

        @pl.when(stage == 0)
        def _():
            pltpu.make_async_copy(here_ref.at[m], local.at[m], local_sem.at[m]).start()
        return 0

    lax.fori_loop(0, count, begin, 0)
    for load in loads:
        load.wait()

    def chunk(m, _):
        onward(m).wait_recv()

        @pl.when(stage == 0)
        def _():
            pltpu.make_async_copy(here_ref.at[m], local.at[m], local_sem.at[m]).wait()
            recv[m] = recv[m] + local[m]

        pltpu.make_async_copy(recv.at[m], save_ref.at[m], save_sem.at[m]).start()
        x = recv[m]
        total = None
        ahead = jnp.dot(x, w1[:, 0:width], preferred_element_type=F32)
        for part in range(PARTS):
            cols = slice(part * width, (part + 1) * width)
            pre = ahead
            if part < PARTS - 1:
                ahead = jnp.dot(x, w1[:, (part + 1) * width:(part + 2) * width], preferred_element_type=F32)
            hidden = gelu_hidden(pre)
            term = jnp.dot(hidden, w2[cols, :], preferred_element_type=F32)
            total = term if total is None else total + term
        out_buf[m] = (x.astype(F32) + total).astype(BF)

        @pl.when(stage < end)
        def _():
            onward(m).start()

        @pl.when(stage == end)
        def _():
            local[m] = norm_f32(out_buf[m]).astype(BF)
            pltpu.make_async_copy(out_buf.at[m], last_ref.at[m], last_sem.at[m]).start()
            pltpu.make_async_copy(local.at[m], n_ref.at[m], n_sem.at[m]).start()
        return 0

    lax.fori_loop(0, count, chunk, 0)

    def finish(m, _):
        pltpu.make_async_copy(recv.at[m], save_ref.at[m], save_sem.at[m]).wait()

        @pl.when(stage == 2)
        def _():
            far(m).wait_send()

        @pl.when(stage < end)
        def _():
            onward(m).wait_send()

        @pl.when(stage == end)
        def _():
            pltpu.make_async_copy(out_buf.at[m], last_ref.at[m], last_sem.at[m]).wait()
            pltpu.make_async_copy(local.at[m], n_ref.at[m], n_sem.at[m]).wait()
        return 0

    lax.fori_loop(0, count, finish, 0)


def forward_pipe(chip_rows, w1, w2):
    count, rows, dim = chip_rows.shape
    any_spec = pl.BlockSpec(memory_space=pl.ANY)
    store = jax.ShapeDtypeStruct(chip_rows.shape, BF)
    dma = pltpu.SemaphoreType.DMA
    return pl.pallas_call(
        forward_pipe_body,
        in_specs=[any_spec] * 3,
        out_specs=[any_spec] * 3,
        out_shape=[store] * 3,
        scratch_shapes=[pltpu.VMEM(chip_rows.shape, BF)] * 3 + [pltpu.VMEM(w1.shape, BF), pltpu.VMEM(w2.shape, BF), dma((2,))] + [dma((count,))] * 7,
        compiler_params=pltpu.CompilerParams(vmem_limit_bytes=PIPE_CAP, has_side_effects=True),
        cost_estimate=pl.CostEstimate(flops=4 * count * rows * dim * w1.shape[1], bytes_accessed=4 * dim * w1.shape[1], transcendentals=0),
        name="forward_pipe",
    )(chip_rows, w1, w2)


def backward_pipe_body(x_ref, top_ref, w1_ref, w1t_ref, w2t_ref, g_ref, h_ref, gp_ref, dx_ref, recv, x_buf, h_buf, gp_buf, gin_buf, w1, w1t, w2t,
                       w_sem, top_sem, x_sem, recv_sem, send_sem, g_sem, h_sem, gp_sem, dx_sem, dx_recv):
    stage = lax.axis_index("stage")
    count = recv.shape[0]
    end = STAGES - 1
    width = w1.shape[1] // PARTS
    loads = [pltpu.make_async_copy(src, dst, w_sem.at[i]) for i, (src, dst) in enumerate(((w1_ref, w1), (w1t_ref, w1t), (w2t_ref, w2t)))]
    for load in loads:
        load.start()

    def load_top(m):
        return pltpu.make_async_copy(top_ref.at[m], recv.at[m], top_sem.at[m])

    def load_x(m):
        return pltpu.make_async_copy(x_ref.at[m], x_buf.at[lax.rem(m, 2)], x_sem.at[m])

    def save_g(m):
        return pltpu.make_async_copy(recv.at[m], g_ref.at[m], g_sem.at[m])

    def save_h(m):
        return pltpu.make_async_copy(h_buf.at[lax.rem(m, 2)], h_ref.at[m], h_sem.at[m])

    def save_gp(m):
        return pltpu.make_async_copy(gp_buf.at[lax.rem(m, 2)], gp_ref.at[m], gp_sem.at[m])

    def save_dx(m):
        return pltpu.make_async_copy(gin_buf.at[lax.rem(m, 2)], dx_ref.at[m], dx_sem.at[m])

    def onward(m):
        return remote(gin_buf.at[lax.rem(m, 2)], recv.at[m], send_sem.at[m], recv_sem.at[m], lax.rem(stage + end, STAGES))

    def cross(m):
        return remote(gin_buf.at[lax.rem(m, 2)], dx_ref.at[m], send_sem.at[m], dx_recv.at[m], 2)

    def begin(m, _):
        @pl.when(stage == end)
        def _():
            load_top(m).start()
        return 0

    lax.fori_loop(0, count, begin, 0)
    load_x(0).start()
    for load in loads:
        load.wait()

    def drain(m):
        save_h(m).wait()
        save_gp(m).wait()

        @pl.when(stage > 0)
        def _():
            onward(m).wait_send()

        @pl.when(stage == 0)
        def _():
            cross(m).wait_send()
            save_dx(m).wait()

    def chunk(m, _):
        slot = lax.rem(m, 2)

        @pl.when(m + 1 < count)
        def _():
            load_x(m + 1).start()

        @pl.when(stage == end)
        def _():
            load_top(m).wait()

        @pl.when(stage < end)
        def _():
            onward(m).wait_recv()

        save_g(m).start()
        load_x(m).wait()

        @pl.when(m >= 2)
        def _():
            drain(m - 2)

        x = x_buf[slot]
        grad_out = recv[m]

        def both(part):
            cols = slice(part * width, (part + 1) * width)
            return (jnp.dot(x, w1[:, cols], preferred_element_type=F32),
                    jnp.dot(grad_out, w2t[:, cols], preferred_element_type=F32))

        total = None
        ahead = both(0)
        for part in range(PARTS):
            cols = slice(part * width, (part + 1) * width)
            pre, grad_hidden = ahead
            if part < PARTS - 1:
                ahead = both(part + 1)
            sq = pre * pre
            inner = jnp.tanh(pre * (GELU_K + (GELU_K * GELU_A) * sq))
            side = 0.5 + 0.5 * inner
            bend = (0.5 - 0.5 * inner * inner) * (GELU_K + (3.0 * GELU_K * GELU_A) * sq)
            h_buf[slot, :, cols] = (pre * side).astype(BF)
            grad_pre = (grad_hidden * (side + pre * bend)).astype(BF)
            gp_buf[slot, :, cols] = grad_pre
            term = jnp.dot(grad_pre, w1t[cols, :], preferred_element_type=F32)
            total = term if total is None else total + term
        gin_buf[slot] = (grad_out.astype(F32) + total).astype(BF)
        save_h(m).start()
        save_gp(m).start()

        @pl.when(stage > 0)
        def _():
            onward(m).start()

        @pl.when(stage == 0)
        def _():
            cross(m).start()
            save_dx(m).start()
        return 0

    lax.fori_loop(0, count, chunk, 0)
    drain(count - 2)
    drain(count - 1)

    def finish(m, _):
        save_g(m).wait()

        @pl.when(stage == 2)
        def _():
            cross(m).wait_recv()
        return 0

    lax.fori_loop(0, count, finish, 0)


def backward_pipe(saved_in, grad_last, w1, w1t, w2t):
    count, rows, dim = saved_in.shape
    ffn = w1.shape[1]
    any_spec = pl.BlockSpec(memory_space=pl.ANY)
    store = jax.ShapeDtypeStruct(saved_in.shape, BF)
    wide = jax.ShapeDtypeStruct((count, rows, ffn), BF)
    dma = pltpu.SemaphoreType.DMA
    return pl.pallas_call(
        backward_pipe_body,
        in_specs=[any_spec] * 5,
        out_specs=[any_spec] * 4,
        out_shape=[store, wide, wide, store],
        scratch_shapes=[
            pltpu.VMEM(saved_in.shape, BF),
            pltpu.VMEM((2, rows, dim), BF),
            pltpu.VMEM((2, rows, ffn), BF),
            pltpu.VMEM((2, rows, ffn), BF),
            pltpu.VMEM((2, rows, dim), BF),
            pltpu.VMEM(w1.shape, BF), pltpu.VMEM(w1t.shape, BF), pltpu.VMEM(w2t.shape, BF),
            dma((3,)),
        ] + [dma((count,))] * 9,
        compiler_params=pltpu.CompilerParams(vmem_limit_bytes=PIPE_CAP, has_side_effects=True),
        cost_estimate=pl.CostEstimate(flops=6 * count * rows * dim * ffn, bytes_accessed=4 * dim * ffn, transcendentals=0),
        name="backward_pipe",
    )(saved_in, grad_last, w1, w1t, w2t)


def head_forward_body(n_valid, scale, n_ref, e_ref, lab_ref, p_ref, m_ref, st_ref, run):
    tile, chunk = pl.program_id(0), pl.program_id(1)

    @pl.when(tile == 0)
    def _():
        run[chunk, 0:1, :] = jnp.full((1, run.shape[2]), -jnp.inf, F32)
        run[chunk, 1:3, :] = jnp.zeros((2, run.shape[2]), F32)

    n_rows = n_ref[0]
    lab = lab_ref[0] - tile * TILE
    top, tot, hit = run[chunk, 0:1, :], run[chunk, 1:2, :], run[chunk, 2:3, :]
    rows = lax.broadcasted_iota(jnp.int32, (SUB, n_rows.shape[0]), 0)
    for sub in range(SUBS):
        cut = slice(sub * SUB, (sub + 1) * SUB)
        logit = lax.dot_general(e_ref[cut, :], n_rows, NT, preferred_element_type=F32) * scale
        if sub == SUBS - 1:
            logit = jnp.where(rows < n_valid - tile * TILE - sub * SUB, logit, -jnp.inf)
        hit = hit + jnp.sum(jnp.where(rows == lab - sub * SUB, logit, 0.0), axis=0, keepdims=True)
        new_top = jnp.maximum(top, jnp.max(logit, axis=0, keepdims=True))
        expo = jnp.exp2(logit - new_top)
        tot = tot * jnp.exp2(top - new_top) + jnp.sum(expo, axis=0, keepdims=True)
        p_ref[0, cut, :] = expo.astype(BF)
        m_ref[0, 0, sub:sub + 1, :] = new_top
        top = new_top
    run[chunk, 0:1, :] = top
    run[chunk, 1:2, :] = tot
    run[chunk, 2:3, :] = hit
    st_ref[0, 0:1, :] = top
    st_ref[0, 1:2, :] = tot
    st_ref[0, 2:3, :] = hit


def transpose_body(n_valid, e_ref, out_ref):
    rows = lax.broadcasted_iota(jnp.int32, e_ref.shape, 0)
    out_ref[...] = jnp.where(rows < n_valid - pl.program_id(0) * e_ref.shape[0], e_ref[...], 0).T


def transposed_table(emb_rows, padded, width=1280):
    n_valid, dim = emb_rows.shape
    return pl.pallas_call(
        functools.partial(transpose_body, n_valid),
        grid=(padded // width,),
        in_specs=[pl.BlockSpec((width, dim), lambda t: (t, 0))],
        out_specs=pl.BlockSpec((dim, width), lambda t: (0, t)),
        out_shape=jax.ShapeDtypeStruct((dim, padded), BF),
        compiler_params=pltpu.CompilerParams(vmem_limit_bytes=VMEM_CAP),
        cost_estimate=pl.CostEstimate(flops=20 * padded * dim, bytes_accessed=4 * padded * dim, transcendentals=0),
        name="table_t",
    )(emb_rows)


def head_forward(normed, emb_rows, labels, scale):
    chunks, rows, dim = normed.shape
    n_valid = emb_rows.shape[0]
    tiles = -(-n_valid // TILE)
    padded = tiles * TILE
    row = pl.BlockSpec((1, 1, rows), lambda t, c: (c, 0, 0))
    return pl.pallas_call(
        functools.partial(head_forward_body, n_valid, scale),
        grid=(tiles, chunks),
        in_specs=[
            pl.BlockSpec((1, rows, dim), lambda t, c: (c, 0, 0)),
            pl.BlockSpec((TILE, dim), lambda t, c: (t, 0)),
            row,
        ],
        out_specs=[
            pl.BlockSpec((1, TILE, rows), lambda t, c: (c, t, 0)),
            pl.BlockSpec((1, 1, SUBS, rows), lambda t, c: (c, t, 0, 0)),
            pl.BlockSpec((1, 3, rows), lambda t, c: (c, 0, 0)),
        ],
        out_shape=[
            jax.ShapeDtypeStruct((chunks, padded, rows), BF),
            jax.ShapeDtypeStruct((chunks, tiles, SUBS, rows), F32),
            jax.ShapeDtypeStruct((chunks, 3, rows), F32),
        ],
        scratch_shapes=[pltpu.VMEM((chunks, 3, rows), F32)],
        compiler_params=pltpu.CompilerParams(vmem_limit_bytes=VMEM_CAP),
        cost_estimate=pl.CostEstimate(flops=2 * chunks * rows * dim * padded, bytes_accessed=padded * (2 * dim + 2 * rows * chunks), transcendentals=rows * chunks * padded),
        name="head_fwd",
    )(normed, emb_rows, labels)


def head_backward_body(p_ref, c_ref, lab_ref, g_ref, et_ref, d_ref, out_ref, acc_ref):
    tile, chunk = pl.program_id(0), pl.program_id(1)
    lab = lab_ref[0] - tile * TILE
    gain = g_ref[0]
    rows = lax.broadcasted_iota(jnp.int32, (SUB, lab.shape[1]), 0)
    def delta_of(sub):
        cut = slice(sub * SUB, (sub + 1) * SUB)
        prob = p_ref[0, cut, :].astype(F32) * c_ref[0, 0, sub:sub + 1, :]
        delta = jnp.where(rows == lab - sub * SUB, gain, prob).astype(BF)
        d_ref[0, cut, :] = delta
        return delta

    total = None
    ahead = delta_of(0)
    for sub in range(SUBS):
        delta = ahead
        if sub < SUBS - 1:
            ahead = delta_of(sub + 1)
        term = jnp.dot(et_ref[:, sub * SUB:(sub + 1) * SUB], delta, preferred_element_type=F32)
        total = term if total is None else total + term

    @pl.when(tile == 0)
    def _():
        acc_ref[chunk] = total

    @pl.when(tile > 0)
    def _():
        acc_ref[chunk] += total

    @pl.when(tile == pl.num_programs(0) - 1)
    def _():
        out_ref[0] = acc_ref[chunk].T.astype(BF)


def head_backward(expo, coef, labels, gain, emb_t):
    chunks, padded, rows = expo.shape
    dim = emb_t.shape[0]
    tiles = padded // TILE
    row = pl.BlockSpec((1, 1, rows), lambda t, c: (c, 0, 0))
    block = pl.BlockSpec((1, TILE, rows), lambda t, c: (c, t, 0))
    end = tiles - 1
    return pl.pallas_call(
        head_backward_body,
        grid=(tiles, chunks),
        in_specs=[
            block,
            pl.BlockSpec((1, 1, SUBS, rows), lambda t, c: (c, t, 0, 0)),
            row,
            row,
            pl.BlockSpec((dim, TILE), lambda t, c: (0, t)),
        ],
        out_specs=[block, pl.BlockSpec((1, rows, dim), lambda t, c: (c * (t // end), 0, 0))],
        out_shape=[jax.ShapeDtypeStruct(expo.shape, BF), jax.ShapeDtypeStruct((chunks, rows, dim), BF)],
        scratch_shapes=[pltpu.VMEM((chunks, dim, rows), F32)],
        input_output_aliases={0: 0},
        compiler_params=pltpu.CompilerParams(vmem_limit_bytes=VMEM_CAP),
        cost_estimate=pl.CostEstimate(flops=2 * chunks * rows * dim * padded, bytes_accessed=padded * (2 * dim + 4 * rows * chunks), transcendentals=0),
        name="head_bwd",
    )(expo, coef, labels, gain, emb_t)


def table_grad_body(groups, *refs):
    deltas, normed, out_ref = refs[:groups], refs[groups:2 * groups], refs[2 * groups]
    total = None
    for d_ref, n_ref in zip(deltas, normed):
        for chunk in range(d_ref.shape[0]):
            term = jnp.dot(d_ref[chunk], n_ref[chunk], preferred_element_type=F32)
            total = term if total is None else total + term
    out_ref[...] = total


def table_grad(deltas, normed, slice_rows, v_tile):
    _, rows, dim = normed[0].shape
    groups = len(deltas)
    tokens = sum(part.shape[0] for part in normed) * rows
    return pl.pallas_call(
        functools.partial(table_grad_body, groups),
        grid=(-(-slice_rows // v_tile),),
        in_specs=[pl.BlockSpec((part.shape[0], v_tile, rows), lambda v: (0, v, 0)) for part in deltas]
        + [pl.BlockSpec(part.shape, lambda v: (0, 0, 0), pipeline_mode=pl.Buffered(1)) for part in normed],
        out_specs=pl.BlockSpec((v_tile, dim), lambda v: (v, 0)),
        out_shape=jax.ShapeDtypeStruct((slice_rows, dim), F32),
        compiler_params=pltpu.CompilerParams(vmem_limit_bytes=VMEM_CAP),
        cost_estimate=pl.CostEstimate(flops=2 * slice_rows * dim * tokens, bytes_accessed=2 * slice_rows * tokens, transcendentals=0),
        name="table_grad",
    )(*deltas, *normed)


def norm_back_body(part_ref, near_ref, far_ref, act_ref, *refs):
    grad = part_ref[0].astype(F32) + near_ref[0].astype(F32) + far_ref[0].astype(F32)
    act = act_ref[0].astype(F32)
    inv = lax.rsqrt(jnp.mean(act * act, axis=-1, keepdims=True) + NORM_EPS)
    along = jnp.mean(act * grad, axis=-1, keepdims=True) * (inv * inv)
    refs[-1][0] = (inv * (grad - act * along)).astype(BF)


def norm_back(part, near, far, last_out, first, store):
    count, rows, dim = part.shape
    here = pl.BlockSpec((1, rows, dim), lambda c: (c, 0, 0))
    there = pl.BlockSpec((1, rows, dim), lambda c: (c + first, 0, 0))
    extra = [] if store is None else [store]
    return pl.pallas_call(
        norm_back_body,
        grid=(count,),
        in_specs=[here, here, here, there] + [pl.BlockSpec(memory_space=pl.ANY)] * len(extra),
        out_specs=there,
        out_shape=jax.ShapeDtypeStruct(last_out.shape, BF),
        input_output_aliases={4: 0} if extra else {},
        compiler_params=pltpu.CompilerParams(vmem_limit_bytes=VMEM_CAP),
        cost_estimate=pl.CostEstimate(flops=20 * part.size, bytes_accessed=10 * part.size, transcendentals=0),
        name="norm_back",
    )(part, near, far, last_out, *extra)


def solution(mesh):

    def stage_body(token_ids, label_ids, emb_rows, w_in, w_out):
        stage = lax.axis_index("stage")
        micro_count, micro_tokens = token_ids.shape
        slice_rows, dim = emb_rows.shape
        scale = dim ** -0.5
        w1, w2 = w_in[0], w_out[0]
        row_start = stage * slice_rows
        padded = -(-slice_rows // TILE) * TILE
        unit = micro_count // CUTS[-1]

        def hop(value, *pairs):
            return lax.ppermute(value, "stage", pairs)

        local_tok = token_ids - row_start
        tok_here = (local_tok >= 0) & (local_tok < slice_rows)
        looked_up = jnp.take(emb_rows, jnp.clip(local_tok, 0, slice_rows - 1), axis=0)
        own_rows = jnp.where(tok_here[..., None], looked_up, 0)
        chip_rows = own_rows + hop(own_rows, (1, 0), (3, 2))

        emb_t = transposed_table(emb_rows, padded)
        local_lab = label_ids - row_start
        labels = jnp.where((local_lab >= 0) & (local_lab < slice_rows), local_lab, -1)[:, None]

        fine = (micro_count * SPLIT, micro_tokens // SPLIT, dim)
        saved_in, last_out, normed = forward_pipe(chip_rows.reshape(fine), w1, w2)
        last_out = last_out.reshape(chip_rows.shape)
        normed = normed.reshape(chip_rows.shape)

        cuts = [slice(lo * unit, hi * unit) for lo, hi in zip(CUTS[:-1], CUTS[1:])]
        n_parts, expo, maxes, stats = [], [], [], []
        for g, cut in enumerate(cuts):
            own = normed[cut]
            if g > 0:
                own, n_parts[-1] = lax.optimization_barrier((own, n_parts[-1]))
            near = hop(own, (3, 2))
            cross = hop(own, (3, 1))
            relay = cross
            if g > 0:
                relay, stats[-1] = lax.optimization_barrier((cross, stats[-1]))
            final = hop(relay, (1, 0))
            part = jnp.where(stage == 3, own, jnp.where(stage == 2, near, jnp.where(stage == 1, relay, final)))
            res = head_forward(part, emb_rows, labels[cut], scale * LOG2E)
            n_parts.append(part)
            expo.append(res[0])
            maxes.append(res[1])
            stats.append(res[2])

        every = lax.all_gather(jnp.concatenate(stats), "stage")
        top = jnp.max(every[:, :, 0], axis=0)
        denom = jnp.sum(every[:, :, 1] * jnp.exp2(every[:, :, 0] - top), axis=0)
        hit = jnp.sum(every[:, :, 2], axis=0)
        mean_loss = (jnp.sum(jnp.log2(denom) + top - hit) * (LN2 / (micro_count * micro_tokens))).reshape(1)
        ratio = scale / denom
        gain = ((jnp.exp2(hit - top) / denom - 1.0) * scale)[:, None]

        deltas, parts, nears, sent = [], [], [], []
        for g, cut in enumerate(cuts):
            coef = jnp.exp2(maxes[g] - top[cut, None, None]) * ratio[cut, None, None]
            delta, part = head_backward(expo[g], coef, labels[cut], gain[cut], emb_t)
            if g >= 2:
                part, sent[g - 2] = lax.optimization_barrier((part, sent[g - 2]))
            near = hop(part, (0, 1), (2, 3))
            deltas.append(delta)
            parts.append(part)
            nears.append(near)
            sent.append((part.astype(F32) + near.astype(F32)).astype(BF))
        deltas, sent = lax.optimization_barrier((deltas, sent))
        far = [hop(value, (1, 3)) for value in sent]
        grad_head = table_grad(deltas, n_parts, slice_rows, V_TILE)
        far, grad_head = lax.optimization_barrier((far, grad_head))
        grad_last = None
        for g, cut in enumerate(cuts):
            grad_last = norm_back(parts[g], nears[g], far[g], last_out, cut.start, grad_last)

        grads, hidden, grad_pre, dx_rows = backward_pipe(saved_in, grad_last.reshape(fine), w1, w1.T, w2.T)
        dx_rows = dx_rows.reshape(chip_rows.shape)

        def flat(value):
            return value.reshape(-1, value.shape[2])

        grad_first = jnp.einsum("td,tf->df", flat(saved_in), flat(grad_pre), preferred_element_type=F32)
        grad_second = jnp.einsum("tf,td->fd", flat(hidden), flat(grads), preferred_element_type=F32)
        dx_rows = jnp.where(stage % 2 == 0, dx_rows, hop(dx_rows, (0, 1), (2, 3)))
        seg = jnp.where(tok_here, local_tok, slice_rows).reshape(-1)
        grad_emb = grad_head.at[seg].add(dx_rows.reshape(-1, dim).astype(F32), mode="drop")
        return mean_loss, grad_first[None], grad_second[None], grad_emb

    return jax.shard_map(
        stage_body,
        mesh=mesh,
        in_specs=(P("dp", None), P("dp", None), P("stage", None), P("stage", None, None), P("stage", None, None)),
        out_specs=(P("dp"), P(("dp", "stage"), None, None), P(("dp", "stage"), None, None), P(("dp", "stage"), None)),
        check_vma=False,
    )
```
